512 devices in a mesh: scen: 32 (over z, core), grp: 16 (over x, y).
Axes of the slice: x: 4, y: 4, z: 16, core: 2. Of those that a mesh axis runs over, the one named last changes fastest.
Arguments:
- borders: bfloat16 [192, 512, 2048], P('scen', None, 'grp'), may hold values from -0.25 to 0.25
- row_scale: float32 [192, 512], P('scen'), may hold values from 0.1 to 10
- assign: int32 [192], P('scen'), may hold values from 0 to 191, each once
- prob: float32 [192], replicated, may hold values from 0.5 to 2
- pattern: int32 [192, 16], replicated, may hold values 0 or 1
- first_diag: float32 [2048], replicated, may hold values from 0.1 to 2
- rhs: float32 [2048], replicated, may hold values from -6 to 6
Outputs:
- schur: float32 [2048, 2048], P('scen', 'grp')
- solution: float32 [2048], replicated
The draws below stay inside these ranges and needn't reach their ends.
Inputs may be any that keep to these rules, and one draw needn't show every extreme that they name: `assign`: each scenario number appears in exactly one slot.
All inputs are finite; a program needn't handle non-finite values.
Results may differ from the reference program's by a relative error of at most 0.00053.
Values may be sent and summed in bfloat16 or wider, within the bound.
A program may use at most 64 MiB of HBM per device.

```python
import math
import jax
import jax.numpy as jnp
from jax import lax

NF = 2048
R = 512
NT = 16
ITERS = 5
SC_DEV = 6
SCEN = 192
TILE = 128


def place_ends(drawn, own_key, least, high):
    spot = [jax.random.randint(jax.random.fold_in(own_key, axis), (), 0, length) for axis, length in enumerate(drawn.shape)]
    widest = drawn.shape.index(max(drawn.shape))
    next_to = spot[:widest] + [(spot[widest] + 1) % drawn.shape[widest]] + spot[widest + 1:]
    return drawn.at[tuple(spot)].set(least).at[tuple(next_to)].set(high)


def shard_levels(stream_key, extent, cuts, smallest, largest):
    level, own = 1.0, jax.random.fold_in(stream_key, 6)
    for dim, blocks in cuts:
        draws = jnp.exp(jax.random.uniform(jax.random.fold_in(own, dim), (blocks,), jnp.float32, smallest / len(cuts), largest / len(cuts)))
        level = level * jnp.repeat(draws, extent[dim] // blocks).reshape([-1 if axis == dim else 1 for axis in range(len(extent))])
    return level


def noise(rng, extent, deviation, limit, split=(), held_as=jnp.bfloat16):
    values = deviation * jax.random.normal(rng, extent, jnp.float32)
    if split:
        values = values * shard_levels(rng, extent, split, -0.22, 0.18)
    return jnp.clip(values, -limit, limit).astype(held_as)


def setup_inputs(seed: int = 0) -> dict:
    key_of = jax.random.split(jax.random.key(seed), 8)
    borders = noise(key_of[0], (SCEN, R, NF), R ** -0.5, 0.25, ((0, 32), (2, 16)))
    row_scale = jnp.clip(jnp.exp(math.log(10.0) - 4.6051702 * jax.random.uniform(key_of[1], (SCEN, R), jnp.float32) ** shard_levels(key_of[1], (SCEN, R), ((0, 32),), -0.2, 0.2)), 0.1, 10.0)
    assign = jax.random.permutation(key_of[2], SCEN).astype(jnp.int32)
    prob = jnp.clip(jnp.exp(jax.random.uniform(key_of[3], (SCEN,), jnp.float32, math.log(0.5), math.log(2.0))), 0.5, 2.0)
    pattern = place_ends((jax.random.randint(key_of[4], (SCEN, NT), 0, 4) < 3).astype(jnp.int32), jax.random.fold_in(key_of[4], 1), 0, 1)
    first_diag = jnp.clip(jnp.exp(jax.random.uniform(key_of[5], (NF,), jnp.float32, math.log(0.1), math.log(2.0))), 0.1, 2.0)
    rhs = noise(key_of[6], (NF,), 1.0, 6.0, (), jnp.float32)
    return dict(borders=borders, row_scale=row_scale, assign=assign, prob=prob, pattern=pattern, first_diag=first_diag, rhs=rhs)


def reference(borders, row_scale, assign, prob, pattern, first_diag, rhs):
    tiles_of = pattern[assign]
    col_tile = jnp.arange(NF, dtype=jnp.int32) // TILE
    keep = jnp.take(tiles_of, col_tile, axis=1).astype(borders.dtype)
    masked = borders * keep[:, None, :]
    factor = row_scale * (prob[assign] / SCEN)[:, None]
    scaled = (masked.astype(jnp.float32) * factor[:, :, None]).astype(jnp.bfloat16)
    groups = SCEN // SC_DEV
    left = masked.reshape(groups, SC_DEV * R, NF)
    right = scaled.reshape(groups, SC_DEV * R, NF)

    def accumulate(total, pair):
        one, two = pair
        term = jnp.dot(one.astype(jnp.float32).T, two.astype(jnp.float32), precision=lax.Precision.HIGHEST)
        return total + term, None

    total, unused = lax.scan(accumulate, jnp.zeros((NF, NF), jnp.float32), (left, right))
    schur = total + jnp.diag(first_diag)
    solution = jnp.zeros_like(rhs)
    residual = rhs
    direction = rhs
    norm_now = jnp.dot(residual, residual, precision=lax.Precision.HIGHEST)
    for step in range(ITERS):
        image = jnp.dot(schur, direction, precision=lax.Precision.HIGHEST)
        alpha = norm_now / jnp.dot(direction, image, precision=lax.Precision.HIGHEST)
        solution = solution + alpha * direction
        residual = residual - alpha * image
        norm_next = jnp.dot(residual, residual, precision=lax.Precision.HIGHEST)
        direction = residual + (norm_next / norm_now) * direction
        norm_now = norm_next
    return schur, solution
```

```python
import jax
import jax.numpy as jnp
from jax import lax
from jax.experimental import pallas as pl
from jax.experimental.pallas import tpu as pltpu
from jax.sharding import PartitionSpec as P


ITERS = 5
SIDE = 4
DEPTH = 16
KS = 6
R = 512
T = 128
HALF = R // 2
NCHUNK = 16
CROWS = 64
MESH = pl.DeviceIdType.MESH
F32 = jnp.float32
BF16 = jnp.bfloat16


def kernel(
    assign_ref,
    prob_ref,
    pattern_ref,
    b_ref,
    rs_ref,
    fd_ref,
    rhs_ref,
    schur_ref,
    sol_ref,
    rowbuf,
    colbuf,
    fac,
    acc,
    core_in,
    part,
    near_in,
    near_sum,
    far_in,
    mine,
    own_block,
    block,
    dvec,
    msg,
    inbox,
    tally,
    g_send,
    g_recv,
    c_send,
    c_recv,
    na_send,
    na_recv,
    fa_send,
    fa_recv,
    fb_send,
    fb_recv,
    nb_send,
    nb_recv,
    o_send,
    o_recv,
    m_send,
    m_recv,
):
    scen = lax.axis_index("scen")
    grp = lax.axis_index("grp")
    z = scen // 2
    c = lax.rem(scen, 2)
    x = grp // SIDE
    y = lax.rem(grp, SIDE)

    def at(xx, yy, zz, cc):
        return (2 * zz + cc, SIDE * xx + yy)

    def up(v, by, n):
        return lax.rem(v + by, n)

    def remote(src, dst, send, recv, dev):
        return pltpu.make_async_remote_copy(
            src_ref=src, dst_ref=dst, send_sem=send, recv_sem=recv, device_id=dev, device_id_type=MESH
        )

    jl, jh, jx = z // 8, lax.rem(z // 4, 2), lax.rem(z, 4)
    to_z = 4 * x + 2 * c + jl
    out_to = at(jx, y, to_z, jh)
    out_from = at(z // 4, y, (lax.rem(z, 2) * 2 + c) * 4 + x, lax.rem(z, 4) // 2)
    stays = (out_to[0] == scen) & (out_to[1] == grp)

    def plane_peer(i):
        p = lax.rem(2 * grp + c + i, 32)
        return (2 * z + lax.rem(p, 2), p // 2)

    barrier = pltpu.get_barrier_semaphore()

    def greet(i, carry):
        pl.semaphore_signal(barrier, inc=1, device_id=plane_peer(i), device_id_type=MESH)
        return carry

    lax.fori_loop(1, 32, greet, 0)
    for by in (1, 2, 4, 8, 12, 14, 15):
        pl.semaphore_signal(barrier, inc=1, device_id=at(x, y, up(z, by, DEPTH), c), device_id_type=MESH)

    @pl.when(jnp.logical_not(stays))
    def _():
        pl.semaphore_signal(barrier, inc=1, device_id=out_to, device_id_type=MESH)
        pl.semaphore_signal(barrier, inc=1, device_id=out_from, device_id_type=MESH)

    pl.semaphore_wait(barrier, jnp.where(stays, 38, 40))

    xp, xm, yp, ym = up(x, 1, SIDE), up(x, 3, SIDE), up(y, 1, SIDE), up(y, 3, SIDE)

    def own(k):
        return (
            remote(b_ref.at[k], colbuf.at[x, k], g_send.at[0, k], g_recv.at[0, k], at(xp, y, z, c)),
            remote(b_ref.at[k], colbuf.at[x, k], g_send.at[1, k], g_recv.at[1, k], at(xm, y, z, c)),
            remote(b_ref.at[k], rowbuf.at[y, k], g_send.at[4, k], g_recv.at[4, k], at(x, yp, z, c)),
            remote(b_ref.at[k], rowbuf.at[y, k], g_send.at[5, k], g_recv.at[5, k], at(x, ym, z, c)),
        )

    lo, hi = pl.ds(0, HALF), pl.ds(HALF, HALF)

    def onward(k):
        return (
            remote(colbuf.at[xm, k, lo], colbuf.at[xm, k, lo], g_send.at[2, k], g_recv.at[2, k], at(xp, y, z, c)),
            remote(colbuf.at[xp, k, hi], colbuf.at[xp, k, hi], g_send.at[3, k], g_recv.at[3, k], at(xm, y, z, c)),
            remote(rowbuf.at[ym, k, lo], rowbuf.at[ym, k, lo], g_send.at[6, k], g_recv.at[6, k], at(x, yp, z, c)),
            remote(rowbuf.at[yp, k, hi], rowbuf.at[yp, k, hi], g_send.at[7, k], g_recv.at[7, k], at(x, ym, z, c)),
        )

    def arrive_own(k):
        remote(b_ref.at[k], colbuf.at[xm, k], g_send.at[0, k], g_recv.at[0, k], at(xp, y, z, c)).wait_recv()
        remote(b_ref.at[k], colbuf.at[xp, k], g_send.at[1, k], g_recv.at[1, k], at(xm, y, z, c)).wait_recv()
        remote(b_ref.at[k], rowbuf.at[ym, k], g_send.at[4, k], g_recv.at[4, k], at(x, yp, z, c)).wait_recv()
        remote(b_ref.at[k], rowbuf.at[yp, k], g_send.at[5, k], g_recv.at[5, k], at(x, ym, z, c)).wait_recv()

    xo, yo = up(x, 2, SIDE), up(y, 2, SIDE)

    def arrive_onward(k):
        remote(b_ref.at[k, lo], colbuf.at[xo, k, lo], g_send.at[2, k], g_recv.at[2, k], at(xp, y, z, c)).wait_recv()
        remote(b_ref.at[k, hi], colbuf.at[xo, k, hi], g_send.at[3, k], g_recv.at[3, k], at(xm, y, z, c)).wait_recv()
        remote(b_ref.at[k, lo], rowbuf.at[yo, k, lo], g_send.at[6, k], g_recv.at[6, k], at(x, yp, z, c)).wait_recv()
        remote(b_ref.at[k, hi], rowbuf.at[yo, k, hi], g_send.at[7, k], g_recv.at[7, k], at(x, ym, z, c)).wait_recv()

    for k in range(2):
        for copy in own(k):
            copy.start()

    colbuf[x] = b_ref[...]
    rowbuf[y] = b_ref[...]
    across = jnp.transpose(jnp.concatenate([rs_ref[...], jnp.zeros((2, R), F32)], axis=0))
    for k in range(KS):
        weight = prob_ref[assign_ref[k]] / SIDE_SCEN
        fac[k] = jnp.broadcast_to(across[:, k : k + 1] * weight, (R, T))
    acc[...] = jnp.zeros_like(acc)

    def contribute(k):
        who = assign_ref[k]
        left = []
        right = []
        for i in range(SIDE):
            row_on = pattern_ref[who, SIDE * x + i]
            col_on = pattern_ref[who, SIDE * i + y].astype(F32)
            tile = rowbuf[i, k]
            left.append(jnp.where(row_on != 0, tile, jnp.zeros_like(tile)))
            right.append((colbuf[i, k].astype(F32) * col_on * fac[k]).astype(BF16))
        left = jnp.concatenate(left, axis=1)
        right = jnp.concatenate(right, axis=1)
        acc[...] += lax.dot_general(left, right, (((0,), (0,)), ((), ())), preferred_element_type=F32)

    def step(k, carry):
        arrive_own(k)
        for copy in onward(k):
            copy.start()

        @pl.when(k < KS - 2)
        def _():
            for copy in own(k + 2):
                copy.start()

        @pl.when(k > 0)
        def _():
            arrive_onward(k - 1)
            contribute(k - 1)

        return carry

    lax.fori_loop(0, KS, step, 0)
    arrive_onward(KS - 1)
    contribute(KS - 1)

    rows = 2 * T
    swap = remote(
        acc.at[pl.ds(pl.multiple_of((1 - c) * rows, rows), rows)],
        core_in,
        c_send,
        c_recv,
        at(x, y, z, 1 - c),
    )
    swap.start()

    def drain(k, carry):
        for copy in own(k) + onward(k):
            copy.wait_send()
        return carry

    lax.fori_loop(0, KS, drain, 0)
    swap.wait_recv()
    first = pl.multiple_of(c * rows, rows)
    for j in range(NCHUNK):
        r0, c0 = (j // 4) * CROWS, (j % 4) * T
        part[j // 4, j % 4] = (
            acc[pl.ds(pl.multiple_of(first + r0, CROWS), CROWS), c0 : c0 + T] + core_in[r0 : r0 + CROWS, c0 : c0 + T]
        )

    m = lax.rem(z, 4)
    q = z // 4
    q01, q23 = pl.ds(0, 2), pl.ds(2, 2)

    def near_dev(by):
        return at(x, y, up(z, by, DEPTH), c)

    near = (
        remote(part.at[:, lax.rem(m + 1, 4)], near_in.at[0], na_send.at[0], na_recv.at[0], near_dev(1)),
        remote(part.at[:, lax.rem(m + 3, 4)], near_in.at[1], na_send.at[1], na_recv.at[1], near_dev(15)),
        remote(part.at[q01, lax.rem(m + 2, 4)], near_in.at[2, q01], na_send.at[2], na_recv.at[2], near_dev(2)),
        remote(part.at[q23, lax.rem(m + 2, 4)], near_in.at[2, q23], na_send.at[3], na_recv.at[3], near_dev(14)),
    )
    for copy in near:
        copy.start()
    for copy in near:
        copy.wait_recv()
    near_sum[...] = part[:, m] + near_in[0] + near_in[1] + near_in[2]
    far = tuple(
        remote(
            near_sum.at[up(q, s, 4)],
            far_in.at[s - 1],
            fa_send.at[s - 1],
            fa_recv.at[s - 1],
            near_dev(4 * s),
        )
        for s in (1, 2, 3)
    )
    for copy in far:
        copy.start()
    for copy in far:
        copy.wait_recv()
    total = near_sum[q] + far_in[0] + far_in[1] + far_in[2]
    on_diag = (2 * c + jl == y) & (jx == x)
    lane = lax.broadcasted_iota(jnp.int32, (CROWS, T), 1)
    row = lax.broadcasted_iota(jnp.int32, (CROWS, T), 0)
    diag = jnp.broadcast_to(fd_ref[pl.ds(SIDE * x + y, 1), :], (CROWS, T))
    spot = jnp.where(on_diag, row + CROWS * jh, -1)
    total = total + jnp.where(lane == spot, diag, 0.0)
    mine[...] = total
    block[q, m] = total

    place = remote(mine, own_block, o_send, o_recv, out_to)

    @pl.when(jnp.logical_not(stays))
    def _():
        place.start()

    @pl.when(stays)
    def _():
        own_block[...] = total

    spread = tuple(
        remote(mine, block.at[q, m], fb_send.at[s - 1], fb_recv.at[s - 1], near_dev(4 * s)) for s in (1, 2, 3)
    )
    for copy in spread:
        copy.start()
    for s in (1, 2, 3):
        remote(mine, block.at[up(q, 4 - s, 4), m], fb_send.at[s - 1], fb_recv.at[s - 1], near_dev(4 * s)).wait_recv()
    share = (
        remote(block.at[:, m], block.at[:, m], nb_send.at[0], nb_recv.at[0], near_dev(1)),
        remote(block.at[:, m], block.at[:, m], nb_send.at[1], nb_recv.at[1], near_dev(15)),
        remote(block.at[q01, m], block.at[q01, m], nb_send.at[2], nb_recv.at[2], near_dev(2)),
        remote(block.at[q23, m], block.at[q23, m], nb_send.at[3], nb_recv.at[3], near_dev(14)),
    )
    for copy in share:
        copy.start()
    m1, m2, m3 = lax.rem(m + 1, 4), lax.rem(m + 2, 4), lax.rem(m + 3, 4)
    remote(block.at[:, m], block.at[:, m3], nb_send.at[0], nb_recv.at[0], near_dev(1)).wait_recv()
    remote(block.at[:, m], block.at[:, m1], nb_send.at[1], nb_recv.at[1], near_dev(15)).wait_recv()
    remote(block.at[q01, m], block.at[q01, m2], nb_send.at[2], nb_recv.at[2], near_dev(2)).wait_recv()
    remote(block.at[q23, m], block.at[q23, m2], nb_send.at[3], nb_recv.at[3], near_dev(14)).wait_recv()

    def total_of(v):
        return jnp.sum(jnp.sum(jnp.sum(v, axis=0, keepdims=True), axis=1, keepdims=True), axis=2, keepdims=True)

    residual = rhs_ref[...]
    direction = residual
    answer = jnp.zeros_like(residual)
    norm_now = total_of(residual * residual)
    slot = 2 * x + c
    for it in range(ITERS):
        dvec[...] = direction
        for yl in range(2):
            halves = []
            for h in range(2):
                prod = None
                for xc in range(SIDE):
                    d = dvec[2 * xc + y // 2, pl.ds(lax.rem(y, 2), 1), :]
                    term = block[yl * 2 + h, xc] * d
                    prod = term if prod is None else prod + term
                halves.append(prod)
            both = jnp.concatenate(halves, axis=0)
            msg[it, pl.ds(yl, 1), :] = jnp.sum(jnp.transpose(both), axis=0, keepdims=True)

        def tell(i, carry):
            remote(msg.at[it], inbox.at[it, y, slot], m_send.at[it], m_recv.at[it], plane_peer(i)).start()
            return carry

        lax.fori_loop(1, 32, tell, 0)
        inbox[it, y, slot] = msg[it]
        pltpu.make_async_copy(tally, tally, m_recv.at[it]).wait()
        image = inbox[it, 0] + inbox[it, 1] + inbox[it, 2] + inbox[it, 3]
        alpha = norm_now / total_of(direction * image)
        answer = answer + alpha * direction
        if it < ITERS - 1:
            residual = residual - alpha * image
            norm_next = total_of(residual * residual)
            direction = residual + (norm_next / norm_now) * direction
            norm_now = norm_next
    sol_ref[...] = answer

    swap.wait_send()
    for copy in near + far + spread + share:
        copy.wait_send()
    for it in range(ITERS):
        pltpu.make_async_copy(tally, tally, m_send.at[it]).wait()

    @pl.when(jnp.logical_not(stays))
    def _():
        place.wait_send()
        place.wait_recv()

    schur_ref[...] = own_block[...]


SIDE_SCEN = 192


def on_device(borders, row_scale, assign, prob, pattern, first_diag, rhs):
    smem = pl.BlockSpec(memory_space=pltpu.SMEM)
    vmem = pl.BlockSpec(memory_space=pltpu.VMEM)
    dma = pltpu.SemaphoreType.DMA
    schur, answer = pl.pallas_call(
        kernel,
        out_shape=(
            jax.ShapeDtypeStruct((CROWS, T), F32),
            jax.ShapeDtypeStruct((8, 2, T), F32),
        ),
        in_specs=[smem, smem, smem, vmem, vmem, vmem, vmem],
        out_specs=(vmem, vmem),
        scratch_shapes=[
            pltpu.VMEM((SIDE, KS, R, T), BF16),
            pltpu.VMEM((SIDE, KS, R, T), BF16),
            pltpu.VMEM((KS, R, T), F32),
            pltpu.VMEM((SIDE * T, SIDE * T), F32),
            pltpu.VMEM((2 * T, SIDE * T), F32),
            pltpu.VMEM((4, 4, CROWS, T), F32),
            pltpu.VMEM((3, 4, CROWS, T), F32),
            pltpu.VMEM((4, CROWS, T), F32),
            pltpu.VMEM((3, CROWS, T), F32),
            pltpu.VMEM((CROWS, T), F32),
            pltpu.VMEM((CROWS, T), F32),
            pltpu.VMEM((4, 4, CROWS, T), F32),
            pltpu.VMEM((8, 2, T), F32),
            pltpu.VMEM((ITERS, 2, T), F32),
            pltpu.VMEM((ITERS, SIDE, 8, 2, T), F32),
            pltpu.VMEM((31, 2, T), F32),
            dma((8, KS)),
            dma((8, KS)),
            dma,
            dma,
            dma((4,)),
            dma((4,)),
            dma((3,)),
            dma((3,)),
            dma((3,)),
            dma((3,)),
            dma((4,)),
            dma((4,)),
            dma,
            dma,
            dma((ITERS,)),
            dma((ITERS,)),
        ],
        compiler_params=pltpu.CompilerParams(
            collective_id=0, has_side_effects=True, vmem_limit_bytes=48 * 1024 * 1024
        ),
    )(assign, prob, pattern, borders, row_scale, first_diag.reshape(16, T), rhs.reshape(8, 2, T))
    return schur, answer.reshape(2048)


def solution(mesh):
    placed = (P("scen", None, "grp"), P("scen", None), P("scen"), P(), P(), P(), P())
    return jax.shard_map(
        on_device, mesh=mesh, in_specs=placed, out_specs=(P("scen", "grp"), P()), check_vma=False
    )
```

```python
import jax
import jax.numpy as jnp
from jax import lax
from jax.experimental import pallas as pl
from jax.experimental.pallas import tpu as pltpu
from jax.sharding import PartitionSpec as P


ITERS = 5
SIDE = 4
DEPTH = 16
SCEN = 192
KS = 6
R = 512
T = 128
HALF = R // 2
SUB = 32
REL = (0, 1, 3, 2)
NEAR = 3
ORDER = [(0, 0), (0, 1), (0, 2), (1, 0), (1, 1), (1, 2), (2, 0), (2, 1)]
ORDER += [(2, 2), (0, 3), (1, 3), (2, 3), (3, 0), (3, 1), (3, 2), (3, 3)]
INDEX = {where: i for i, where in enumerate(ORDER)}
MESH = pl.DeviceIdType.MESH
F32 = jnp.float32
BF16 = jnp.bfloat16


def kernel(
    assign_hbm,
    prob_hbm,
    pattern_hbm,
    b_hbm,
    rs_hbm,
    fd_hbm,
    rhs_hbm,
    schur_ref,
    sol_ref,
    assign_ref,
    prob_ref,
    pattern_ref,
    rs_ref,
    fd_ref,
    rhs_ref,
    rowbuf,
    colbuf,
    lefts,
    rights,
    fac,
    pat,
    acc,
    core_in,
    part,
    near_in,
    near_sum,
    far_in,
    mine,
    block,
    out_block,
    dvec,
    msg,
    inbox,
    tally,
    in_sem,
    g_send,
    g_recv,
    c_send,
    c_recv,
    na_send,
    na_recv,
    fa_send,
    fa_recv,
    fb_send,
    fb_recv,
    nb_send,
    nb_recv,
    o_send,
    o_recv,
    m_send,
    m_recv,
):
    scen = lax.axis_index("scen")
    grp = lax.axis_index("grp")
    z = scen // 2
    c = lax.rem(scen, 2)
    x = grp // SIDE
    y = lax.rem(grp, SIDE)

    def at(xx, yy, zz, cc):
        return (2 * zz + cc, SIDE * xx + yy)

    def up(v, by, n):
        return lax.rem(v + by, n)

    def remote(src, dst, send, recv, dev):
        return pltpu.make_async_remote_copy(
            src_ref=src, dst_ref=dst, send_sem=send, recv_sem=recv, device_id=dev, device_id_type=MESH
        )

    fetch_tiles = (
        pltpu.make_async_copy(b_hbm, colbuf.at[0], in_sem.at[0]),
        pltpu.make_async_copy(b_hbm, rowbuf.at[0], in_sem.at[1]),
    )
    fetch_small = tuple(
        pltpu.make_async_copy(src, dst, in_sem.at[2 + i])
        for i, (src, dst) in enumerate(
            (
                (assign_hbm, assign_ref),
                (prob_hbm, prob_ref),
                (pattern_hbm, pattern_ref),
                (rs_hbm, rs_ref),
                (fd_hbm, fd_ref),
                (rhs_hbm, rhs_ref),
            )
        )
    )
    for copy in fetch_tiles + fetch_small:
        copy.start()

    xs = [x] + [up(x, by, SIDE) for by in (1, 2, 3)]
    ys = [y] + [up(y, by, SIDE) for by in (1, 2, 3)]
    far_first = sorted(((a, b) for a in range(4) for b in range(4)), key=lambda d: -(min(d[0], 4 - d[0]) + min(d[1], 4 - d[1])))
    plane = []
    for dx, dy in far_first:
        for cc in (c, 1 - c):
            if (dx, dy) != (0, 0) or cc is not c:
                plane.append(at(xs[dx], ys[dy], z, cc))
    deep = {by: at(x, y, up(z, by, DEPTH), c) for by in (1, 2, 4, 8, 12, 14, 15)}

    with jax.named_scope("entry"):
        barrier = pltpu.get_barrier_semaphore()
        for peer in plane + list(deep.values()):
            pl.semaphore_signal(barrier, inc=1, device_id=peer, device_id_type=MESH)
        pl.semaphore_wait(barrier, len(plane) + len(deep))
        for copy in fetch_tiles:
            copy.wait()

    x_next, x_prev, y_next, y_prev = at(xs[1], y, z, c), at(xs[3], y, z, c), at(x, ys[1], z, c), at(x, ys[3], z, c)
    lo, hi = pl.ds(0, HALF), pl.ds(HALF, HALF)

    def hop(buf, kind, src, dst, k, rows, dev):
        return remote(buf.at[src, k, rows], buf.at[dst, k, rows], g_send.at[kind, k], g_recv.at[kind, k], dev)

    every = pl.ds(0, R)

    def own(k):
        return (
            hop(colbuf, 0, 0, 2, k, every, x_next),
            hop(colbuf, 1, 0, 1, k, every, x_prev),
            hop(rowbuf, 2, 0, 2, k, every, y_next),
            hop(rowbuf, 3, 0, 1, k, every, y_prev),
        )

    def onward(k):
        return (
            hop(colbuf, 4, 2, 3, k, lo, x_next),
            hop(colbuf, 5, 1, 3, k, hi, x_prev),
            hop(rowbuf, 6, 2, 3, k, lo, y_next),
            hop(rowbuf, 7, 1, 3, k, hi, y_prev),
        )

    def send_own(k, carry):
        for copy in own(k):
            copy.start()
        return carry

    lax.fori_loop(0, KS, send_own, 0)

    with jax.named_scope("setup"):
        for copy in fetch_small:
            copy.wait()
        across = jnp.transpose(jnp.concatenate([rs_ref[...], jnp.zeros((2, R), F32)], axis=0))
        slots = lax.broadcasted_iota(jnp.int32, (1, SCEN), 1)
        present = pattern_ref[...].astype(F32)
        for k in range(KS):
            held = (slots == assign_ref[:, k : k + 1]).astype(F32)
            weight = jnp.sum(prob_ref[...] * held, axis=1, keepdims=True) / SCEN
            fac[k] = jnp.broadcast_to(across[:, k : k + 1] * weight, (R, T))
            pat[k] = jnp.broadcast_to(jnp.sum(present * held, axis=1, keepdims=True), (16, T))
        acc[...] = jnp.zeros_like(acc)

    def masked(p, k):
        keep = pat[k, pl.ds(SIDE * x + ys[REL[p]], 1), :].astype(BF16)
        return rowbuf[p, k] * keep

    def scaled(p, k):
        keep = pat[k, pl.ds(SIDE * xs[REL[p]] + y, 1), :]
        return (colbuf[p, k].astype(F32) * keep * fac[k]).astype(BF16)

    def product(left, right):
        return lax.dot_general(left, right, (((0,), (0,)), ((), ())), preferred_element_type=F32)

    def gain(value, rows, cols):
        for i, pr in enumerate(rows):
            for j, pc in enumerate(cols):
                for h in range(2):
                    for s in range(2):
                        r0 = T * i + 64 * h + SUB * s
                        acc[INDEX[pr, pc], h, s] += value[r0 : r0 + SUB, T * j : T * j + T]

    def step_a(k, carry):
        for copy in own(k):
            copy.wait_recv()
        for copy in onward(k):
            copy.start()
        for p in range(NEAR):
            lefts[k, :, T * p : T * p + T] = masked(p, k)
            rights[k, :, T * p : T * p + T] = scaled(p, k)
        gain(product(lefts[k], rights[k]), range(NEAR), range(NEAR))
        return carry

    def step_b(k, carry):
        for copy in onward(k):
            copy.wait_recv()
        left, right = masked(3, k), scaled(3, k)
        gain(product(left, jnp.concatenate([rights[k], right], axis=1)), (3,), range(4))
        gain(product(lefts[k], right), range(NEAR), (3,))
        return carry

    m = lax.rem(z, 4)
    q = z // 4
    ms = [m] + [up(m, by, 4) for by in (1, 2, 3)]
    qs = [q] + [up(q, by, 4) for by in (1, 2, 3)]
    front, back = pl.ds(0, 2), pl.ds(2, 2)

    def swap(w):
        tiles = pl.ds(8 * w, 8)
        return remote(acc.at[tiles, 1 - c], core_in.at[tiles], c_send.at[w], c_recv.at[w], at(x, y, z, 1 - c))

    def combine(w):
        swap(w).wait_recv()
        for i in range(8):
            for s in range(2):
                part[w, i // 2, 2 * (i % 2) + s] = acc[8 * w + i, c, s] + core_in[8 * w + i, s]

    def near(w):
        return (
            remote(part.at[w, :, ms[1]], near_in.at[w, 0], na_send.at[w, 0], na_recv.at[w, 0], deep[1]),
            remote(part.at[w, :, ms[3]], near_in.at[w, 1], na_send.at[w, 1], na_recv.at[w, 1], deep[15]),
            remote(part.at[w, front, ms[2]], near_in.at[w, 2, front], na_send.at[w, 2], na_recv.at[w, 2], deep[2]),
            remote(part.at[w, back, ms[2]], near_in.at[w, 2, back], na_send.at[w, 3], na_recv.at[w, 3], deep[14]),
        )

    def near_done(w):
        for copy in near(w):
            copy.wait_recv()
        near_sum[w] = part[w, :, m] + near_in[w, 0] + near_in[w, 1] + near_in[w, 2]

    def far(w):
        return tuple(
            remote(near_sum.at[w, qs[s]], far_in.at[w, s - 1], fa_send.at[w, s - 1], fa_recv.at[w, s - 1], deep[4 * s])
            for s in (1, 2, 3)
        )

    def far_done(w):
        for copy in far(w):
            copy.wait_recv()
        total = near_sum[w, q] + far_in[w, 0] + far_in[w, 1] + far_in[w, 2]
        if w == 0:
            lane = lax.broadcasted_iota(jnp.int32, (SUB, T), 1)
            row = lax.broadcasted_iota(jnp.int32, (SUB, T), 0)
            diag = jnp.broadcast_to(fd_ref[x, pl.ds(y, 1), :], (SUB, T))
            spot = jnp.where(z < 2, row + 64 * c + SUB * lax.rem(z, 2), -1)
            total = total + jnp.where(lane == spot, diag, 0.0)
        mine[w] = total
        block[w, q, m] = total

    def spread(w):
        return tuple(
            remote(mine.at[w], block.at[w, q, m], fb_send.at[w, s - 1], fb_recv.at[w, s - 1], deep[4 * s])
            for s in (1, 2, 3)
        )

    def share(w):
        return tuple(
            remote(block.at[w, sel, m], block.at[w, sel, m], nb_send.at[w, i], nb_recv.at[w, i], deep[by])
            for i, (sel, by) in enumerate(((pl.ds(0, 4), 1), (pl.ds(0, 4), 15), (front, 2), (back, 14)))
        )

    def start(copies):
        for copy in copies:
            copy.start()

    def wait_recv(copies):
        for copy in copies:
            copy.wait_recv()

    with jax.named_scope("gather_a"):
        lax.fori_loop(0, KS, step_a, 0)
    swap(0).start()
    with jax.named_scope("gather_b0"):
        lax.fori_loop(0, 2, step_b, 0)
    with jax.named_scope("swap_a"):
        combine(0)
    start(near(0))
    with jax.named_scope("gather_b1"):
        lax.fori_loop(2, KS, step_b, 0)
    swap(1).start()
    with jax.named_scope("near_a"):
        near_done(0)
    start(far(0))
    with jax.named_scope("swap_b"):
        combine(1)
    start(near(1))
    with jax.named_scope("near_b"):
        near_done(1)
    start(far(1))
    with jax.named_scope("far_a"):
        far_done(0)
    start(spread(0))
    with jax.named_scope("far_b"):
        far_done(1)
    start(spread(1))
    with jax.named_scope("spread_a"):
        wait_recv(spread(0))
    start(share(0))
    with jax.named_scope("spread_b"):
        wait_recv(spread(1))
    start(share(1))
    with jax.named_scope("share_ab"):
        wait_recv(share(0))
        wait_recv(share(1))

    def total_of(v):
        return jnp.sum(jnp.sum(jnp.sum(v, axis=0, keepdims=True), axis=1, keepdims=True), axis=2, keepdims=True)

    def tile_at(idx):
        return idx // 8, lax.rem(idx, 8) // 2, 2 * lax.rem(idx, 2)

    rel = lax.rem(m + SIDE - y, SIDE)
    out_row = jnp.where(rel == 2, 3, jnp.where(rel == 3, 2, rel))
    giver = x == q

    def out_tile(pc):
        idx = INDEX[0, pc]
        for pr in (1, 2, 3):
            idx = jnp.where(out_row == pr, INDEX[pr, pc], idx)
        return tile_at(idx)

    def give(pc):
        w, qq, mm = out_tile(pc)
        dev = at(xs[REL[pc]], y, z, c)
        return remote(block.at[w, qq, pl.ds(mm, 2)], out_block, o_send.at[pc - 1], o_recv, dev)

    residual = rhs_ref[...]
    direction = residual
    answer = jnp.zeros_like(residual)
    norm_now = total_of(residual * residual)
    for it in range(ITERS):
        with jax.named_scope(f"cg{it}"):
            dvec[...] = direction
            for pr in range(4):
                halves = []
                for s in range(2):
                    prod = None
                    for pc in range(4):
                        d = dvec[xs[REL[pc]], pl.ds(y, 1), :]
                        i = INDEX[pr, pc]
                        term = block[i // 8, (i % 8) // 2, 2 * (i % 2) + s] * d
                        prod = term if prod is None else prod + term
                    halves.append(prod)
                both = jnp.concatenate(halves, axis=0)
                placed = [jnp.where(c == h, both, jnp.zeros_like(both)) for h in range(2)]
                line = jnp.sum(jnp.transpose(jnp.concatenate(placed, axis=0)), axis=0, keepdims=True)
                msg[it, pl.ds(ys[REL[pr]], 1), :] = line
            for peer in plane:
                remote(msg.at[it], inbox.at[it, 2 * y + c, x], m_send.at[it], m_recv.at[it], peer).start()
            inbox[it, 2 * y + c, x] = msg[it]
            if it == ITERS - 1:

                @pl.when(giver)
                def _():
                    for pc in (1, 2, 3):
                        give(pc).start()
                    w, qq, mm = out_tile(0)
                    out_block[...] = block[w, qq, pl.ds(mm, 2)]

            pltpu.make_async_copy(tally, tally, m_recv.at[it]).wait()
            image = inbox[it, 0]
            for i in range(1, 8):
                image = image + inbox[it, i]
            alpha = norm_now / total_of(direction * image)
            answer = answer + alpha * direction
            if it < ITERS - 1:
                residual = residual - alpha * image
                norm_next = total_of(residual * residual)
                direction = residual + (norm_next / norm_now) * direction
                norm_now = norm_next
    sol_ref[...] = answer

    with jax.named_scope("finish"):

        @pl.when(jnp.logical_not(giver))
        def _():
            give(1).wait_recv()

        for s in range(2):
            schur_ref[SUB * s : SUB * s + SUB] = out_block[s]

        def drain(k, carry):
            for copy in own(k) + onward(k):
                copy.wait_send()
            return carry

        lax.fori_loop(0, KS, drain, 0)
        for w in range(2):
            swap(w).wait_send()
            for copy in near(w) + far(w) + spread(w) + share(w):
                copy.wait_send()
        for it in range(ITERS):
            pltpu.make_async_copy(tally, tally, m_send.at[it]).wait()

        @pl.when(giver)
        def _():
            for pc in (1, 2, 3):
                give(pc).wait_send()


def on_device(borders, row_scale, assign, prob, pattern, first_diag, rhs):
    held = pl.BlockSpec(memory_space=pltpu.HBM)
    vmem = pl.BlockSpec(memory_space=pltpu.VMEM)
    dma = pltpu.SemaphoreType.DMA
    schur, answer = pl.pallas_call(
        kernel,
        out_shape=(
            jax.ShapeDtypeStruct((2 * SUB, T), F32),
            jax.ShapeDtypeStruct((SIDE, SIDE, T), F32),
        ),
        in_specs=[held] * 7,
        out_specs=(vmem, vmem),
        scratch_shapes=[
            pltpu.VMEM((1, KS), jnp.int32),
            pltpu.VMEM((1, SCEN), F32),
            pltpu.VMEM((16, SCEN), jnp.int32),
            pltpu.VMEM((KS, R), F32),
            pltpu.VMEM((SIDE, SIDE, T), F32),
            pltpu.VMEM((SIDE, SIDE, T), F32),
            pltpu.VMEM((4, KS, R, T), BF16),
            pltpu.VMEM((4, KS, R, T), BF16),
            pltpu.VMEM((KS, R, NEAR * T), BF16),
            pltpu.VMEM((KS, R, NEAR * T), BF16),
            pltpu.VMEM((KS, R, T), F32),
            pltpu.VMEM((KS, 16, T), F32),
            pltpu.VMEM((16, 2, 2, SUB, T), F32),
            pltpu.VMEM((16, 2, SUB, T), F32),
            pltpu.VMEM((2, 4, 4, SUB, T), F32),
            pltpu.VMEM((2, 3, 4, SUB, T), F32),
            pltpu.VMEM((2, 4, SUB, T), F32),
            pltpu.VMEM((2, 3, SUB, T), F32),
            pltpu.VMEM((2, SUB, T), F32),
            pltpu.VMEM((2, 4, 4, SUB, T), F32),
            pltpu.VMEM((2, SUB, T), F32),
            pltpu.VMEM((SIDE, SIDE, T), F32),
            pltpu.VMEM((ITERS, SIDE, T), F32),
            pltpu.VMEM((ITERS, 8, SIDE, SIDE, T), F32),
            pltpu.VMEM((31, SIDE, T), F32),
            dma((8,)),
            dma((8, KS)),
            dma((8, KS)),
            dma((2,)),
            dma((2,)),
            dma((2, 4)),
            dma((2, 4)),
            dma((2, 3)),
            dma((2, 3)),
            dma((2, 3)),
            dma((2, 3)),
            dma((2, 4)),
            dma((2, 4)),
            dma((3,)),
            dma,
            dma((ITERS,)),
            dma((ITERS,)),
        ],
        compiler_params=pltpu.CompilerParams(
            collective_id=0, has_side_effects=True, vmem_limit_bytes=67_043_328
        ),
    )(
        assign.reshape(1, KS),
        prob.reshape(1, SCEN),
        pattern.T,
        borders,
        row_scale,
        first_diag.reshape(SIDE, SIDE, T),
        rhs.reshape(SIDE, SIDE, T),
    )
    return schur, answer.reshape(SIDE * SIDE * T)


def solution(mesh):
    placed = (P("scen", None, "grp"), P("scen", None), P("scen"), P(), P(), P(), P())
    return jax.shard_map(
        on_device, mesh=mesh, in_specs=placed, out_specs=(P("scen", "grp"), P()), check_vma=False
    )
```

```python
import jax
import jax.numpy as jnp
from jax import lax
from jax.experimental import pallas as pl
from jax.experimental.pallas import tpu as pltpu
from jax.sharding import PartitionSpec as P


ITERS = 5
EARLY = 2
SIDE = 4
DEPTH = 16
SCEN = 192
KS = 6
R = 512
T = 128
HALF = R // 2
SUB = 32
REL = (0, 1, 3, 2)
NEAR = 3
ORDER = [(0, 0), (0, 1), (0, 2), (1, 0), (1, 1), (1, 2), (2, 0), (2, 1)]
ORDER += [(2, 2), (0, 3), (1, 3), (2, 3), (3, 0), (3, 1), (3, 2), (3, 3)]
INDEX = {where: i for i, where in enumerate(ORDER)}
MESH = pl.DeviceIdType.MESH
F32 = jnp.float32
BF16 = jnp.bfloat16


def kernel(
    assign_hbm,
    prob_hbm,
    pattern_hbm,
    b_hbm,
    rs_hbm,
    fd_hbm,
    rhs_hbm,
    schur_ref,
    sol_ref,
    assign_ref,
    prob_ref,
    pattern_ref,
    rs_ref,
    fd_ref,
    rhs_ref,
    rowbuf,
    colbuf,
    lefts,
    rights,
    fac,
    pat,
    acc,
    core_in,
    part,
    near_in,
    near_sum,
    far_in,
    mine,
    block,
    out_block,
    dvec,
    msg,
    inbox,
    zmsg,
    zbox,
    tally,
    in_sem,
    g_send,
    g_recv,
    c_send,
    c_recv,
    na_send,
    na_recv,
    fa_send,
    fa_recv,
    fb_send,
    fb_recv,
    nb_send,
    nb_recv,
    o_send,
    o_recv,
    m_send,
    m_recv,
    z_send,
    z_recv,
):
    scen = lax.axis_index("scen")
    grp = lax.axis_index("grp")
    z = scen // 2
    c = lax.rem(scen, 2)
    x = grp // SIDE
    y = lax.rem(grp, SIDE)

    def at(xx, yy, zz, cc):
        return (2 * zz + cc, SIDE * xx + yy)

    def up(v, by, n):
        return lax.rem(v + by, n)

    def remote(src, dst, send, recv, dev):
        return pltpu.make_async_remote_copy(
            src_ref=src, dst_ref=dst, send_sem=send, recv_sem=recv, device_id=dev, device_id_type=MESH
        )

    fetch_tiles = (
        pltpu.make_async_copy(b_hbm, colbuf.at[0], in_sem.at[0]),
        pltpu.make_async_copy(b_hbm, rowbuf.at[0], in_sem.at[1]),
    )
    fetch_small = tuple(
        pltpu.make_async_copy(src, dst, in_sem.at[2 + i])
        for i, (src, dst) in enumerate(
            (
                (assign_hbm, assign_ref),
                (prob_hbm, prob_ref),
                (pattern_hbm, pattern_ref),
                (rs_hbm, rs_ref),
                (fd_hbm, fd_ref),
                (rhs_hbm, rhs_ref),
            )
        )
    )
    for copy in fetch_tiles + fetch_small:
        copy.start()

    xs = [x] + [up(x, by, SIDE) for by in (1, 2, 3)]
    ys = [y] + [up(y, by, SIDE) for by in (1, 2, 3)]
    far_first = sorted(((a, b) for a in range(4) for b in range(4)), key=lambda d: -(min(d[0], 4 - d[0]) + min(d[1], 4 - d[1])))
    plane = []
    for dx, dy in far_first:
        for cc in (c, 1 - c):
            if (dx, dy) != (0, 0) or cc is not c:
                plane.append(at(xs[dx], ys[dy], z, cc))
    deep = {by: at(x, y, up(z, by, DEPTH), c) for by in range(1, DEPTH)}

    with jax.named_scope("entry"):
        barrier = pltpu.get_barrier_semaphore()
        for peer in plane + list(deep.values()):
            pl.semaphore_signal(barrier, inc=1, device_id=peer, device_id_type=MESH)
        pl.semaphore_wait(barrier, len(plane) + len(deep))
        for copy in fetch_tiles:
            copy.wait()

    x_next, x_prev, y_next, y_prev = at(xs[1], y, z, c), at(xs[3], y, z, c), at(x, ys[1], z, c), at(x, ys[3], z, c)
    lo, hi = pl.ds(0, HALF), pl.ds(HALF, HALF)

    def hop(buf, kind, src, dst, k, rows, dev):
        return remote(buf.at[src, k, rows], buf.at[dst, k, rows], g_send.at[kind, k], g_recv.at[kind, k], dev)

    every = pl.ds(0, R)

    def own(k):
        return (
            hop(colbuf, 0, 0, 2, k, every, x_next),
            hop(colbuf, 1, 0, 1, k, every, x_prev),
            hop(rowbuf, 2, 0, 2, k, every, y_next),
            hop(rowbuf, 3, 0, 1, k, every, y_prev),
        )

    def onward(k):
        return (
            hop(colbuf, 4, 2, 3, k, lo, x_next),
            hop(colbuf, 5, 1, 3, k, hi, x_prev),
            hop(rowbuf, 6, 2, 3, k, lo, y_next),
            hop(rowbuf, 7, 1, 3, k, hi, y_prev),
        )

    def send_own(k, carry):
        for copy in own(k):
            copy.start()
        return carry

    lax.fori_loop(0, KS, send_own, 0)

    with jax.named_scope("setup"):
        for copy in fetch_small:
            copy.wait()
        across = jnp.transpose(jnp.concatenate([rs_ref[...], jnp.zeros((2, R), F32)], axis=0))
        slots = lax.broadcasted_iota(jnp.int32, (1, SCEN), 1)
        present = pattern_ref[...].astype(F32)
        for k in range(KS):
            held = (slots == assign_ref[:, k : k + 1]).astype(F32)
            weight = jnp.sum(prob_ref[...] * held, axis=1, keepdims=True) / SCEN
            fac[k] = jnp.broadcast_to(across[:, k : k + 1] * weight, (R, T))
            pat[k] = jnp.broadcast_to(jnp.sum(present * held, axis=1, keepdims=True), (16, T))
        acc[...] = jnp.zeros_like(acc)

    def masked(p, k):
        keep = pat[k, pl.ds(SIDE * x + ys[REL[p]], 1), :].astype(BF16)
        return rowbuf[p, k] * keep

    def scaled(p, k):
        keep = pat[k, pl.ds(SIDE * xs[REL[p]] + y, 1), :]
        return (colbuf[p, k].astype(F32) * keep * fac[k]).astype(BF16)

    def product(left, right):
        return lax.dot_general(left, right, (((0,), (0,)), ((), ())), preferred_element_type=F32)

    def gain(value, rows, cols):
        for i, pr in enumerate(rows):
            for j, pc in enumerate(cols):
                for h in range(2):
                    for s in range(2):
                        r0 = T * i + 64 * h + SUB * s
                        acc[INDEX[pr, pc], h, s] += value[r0 : r0 + SUB, T * j : T * j + T]

    def step_a(k, carry):
        for copy in own(k):
            copy.wait_recv()
        for copy in onward(k):
            copy.start()
        for p in range(NEAR):
            lefts[k, :, T * p : T * p + T] = masked(p, k)
            rights[k, :, T * p : T * p + T] = scaled(p, k)
        gain(product(lefts[k], rights[k]), range(NEAR), range(NEAR))
        return carry

    def step_b(k, carry):
        for copy in onward(k):
            copy.wait_recv()
        left, right = masked(3, k), scaled(3, k)
        gain(product(left, jnp.concatenate([rights[k], right], axis=1)), (3,), range(4))
        gain(product(lefts[k], right), range(NEAR), (3,))
        return carry

    m = lax.rem(z, 4)
    q = z // 4
    ms = [m] + [up(m, by, 4) for by in (1, 2, 3)]
    qs = [q] + [up(q, by, 4) for by in (1, 2, 3)]
    front, back = pl.ds(0, 2), pl.ds(2, 2)

    def swap(w):
        tiles = pl.ds(8 * w, 8)
        return remote(acc.at[tiles, 1 - c], core_in.at[tiles], c_send.at[w], c_recv.at[w], at(x, y, z, 1 - c))

    def combine(w):
        swap(w).wait_recv()
        for i in range(8):
            for s in range(2):
                part[w, i // 2, 2 * (i % 2) + s] = acc[8 * w + i, c, s] + core_in[8 * w + i, s]

    def near(w):
        return (
            remote(part.at[w, :, ms[1]], near_in.at[w, 0], na_send.at[w, 0], na_recv.at[w, 0], deep[1]),
            remote(part.at[w, :, ms[3]], near_in.at[w, 1], na_send.at[w, 1], na_recv.at[w, 1], deep[15]),
            remote(part.at[w, front, ms[2]], near_in.at[w, 2, front], na_send.at[w, 2], na_recv.at[w, 2], deep[2]),
            remote(part.at[w, back, ms[2]], near_in.at[w, 2, back], na_send.at[w, 3], na_recv.at[w, 3], deep[14]),
        )

    def near_done(w):
        for copy in near(w):
            copy.wait_recv()
        near_sum[w] = part[w, :, m] + near_in[w, 0] + near_in[w, 1] + near_in[w, 2]

    def far(w):
        return tuple(
            remote(near_sum.at[w, qs[s]], far_in.at[w, s - 1], fa_send.at[w, s - 1], fa_recv.at[w, s - 1], deep[4 * s])
            for s in (1, 2, 3)
        )

    def far_done(w):
        for copy in far(w):
            copy.wait_recv()
        total = near_sum[w, q] + far_in[w, 0] + far_in[w, 1] + far_in[w, 2]
        if w == 0:
            lane = lax.broadcasted_iota(jnp.int32, (SUB, T), 1)
            row = lax.broadcasted_iota(jnp.int32, (SUB, T), 0)
            diag = jnp.broadcast_to(fd_ref[x, pl.ds(y, 1), :], (SUB, T))
            spot = jnp.where(z < 2, row + 64 * c + SUB * lax.rem(z, 2), -1)
            total = total + jnp.where(lane == spot, diag, 0.0)
        mine[w] = total
        block[w, q, m] = total

    def spread(w):
        return tuple(
            remote(mine.at[w], block.at[w, q, m], fb_send.at[w, s - 1], fb_recv.at[w, s - 1], deep[4 * s])
            for s in (1, 2, 3)
        )

    def share(w):
        return tuple(
            remote(block.at[w, sel, m], block.at[w, sel, m], nb_send.at[w, i], nb_recv.at[w, i], deep[by])
            for i, (sel, by) in enumerate(((pl.ds(0, 4), 1), (pl.ds(0, 4), 15), (front, 2), (back, 14)))
        )

    def start(copies):
        for copy in copies:
            copy.start()

    def wait_recv(copies):
        for copy in copies:
            copy.wait_recv()

    def total_of(v):
        return jnp.sum(jnp.sum(jnp.sum(v, axis=0, keepdims=True), axis=1, keepdims=True), axis=2, keepdims=True)

    def share_of(direction, tile, pieces):
        dvec[...] = direction
        lines = []
        for pr in range(4):
            stack = []
            for piece in pieces:
                prod = None
                for pc in range(4):
                    term = tile(INDEX[pr, pc], piece) * dvec[xs[REL[pc]], pl.ds(y, 1), :]
                    prod = term if prod is None else prod + term
                stack.append(prod)
            both = jnp.concatenate(stack, axis=0)
            if len(pieces) == 2:
                both = jnp.concatenate([jnp.where(c == h, both, jnp.zeros_like(both)) for h in range(2)], axis=0)
            lines.append(jnp.sum(jnp.transpose(both), axis=0, keepdims=True))
        return lines

    def write_lines(ref, it, lines):
        for pr in range(4):
            ref[it, pl.ds(ys[REL[pr]], 1), :] = lines[pr]

    def tell(it):
        for peer in plane:
            remote(msg.at[it], inbox.at[it, 2 * y + c, x], m_send.at[it], m_recv.at[it], peer).start()
        inbox[it, 2 * y + c, x] = msg[it]

    def heard(it):
        pltpu.make_async_copy(tally, tally, m_recv.at[it]).wait()
        image = inbox[it, 0]
        for i in range(1, 8):
            image = image + inbox[it, i]
        return image

    deep_tally = tally.at[pl.ds(0, DEPTH - 1)]

    def early_begin(it, state):
        lines = share_of(state[2], lambda i, p: acc[i, p // 2, p % 2], range(4))
        write_lines(zmsg, it, lines)
        for by in (8, 7, 9, 6, 10, 5, 11, 4, 12, 3, 13, 2, 14, 1, 15):
            remote(zmsg.at[it], zbox.at[it, z], z_send.at[it], z_recv.at[it], deep[by]).start()
        zbox[it, z] = zmsg[it]

    def early_middle(it):
        pltpu.make_async_copy(deep_tally, deep_tally, z_recv.at[it]).wait()
        total = zbox[it, 0]
        for i in range(1, DEPTH):
            total = total + zbox[it, i]
        msg[it] = total
        tell(it)

    def update(it, state, image):
        answer, residual, direction, norm_now = state
        alpha = norm_now / total_of(direction * image)
        answer = answer + alpha * direction
        if it == ITERS - 1:
            return answer, residual, direction, norm_now
        residual = residual - alpha * image
        norm_next = total_of(residual * residual)
        return answer, residual, residual + (norm_next / norm_now) * direction, norm_next

    def early_end(it, state):
        return update(it, state, heard(it) + fd_ref[...] * state[2])

    with jax.named_scope("gather_a"):
        lax.fori_loop(0, KS, step_a, 0)
    swap(0).start()
    with jax.named_scope("gather_b0"):
        lax.fori_loop(0, 2, step_b, 0)
    with jax.named_scope("swap_a"):
        combine(0)
    start(near(0))
    with jax.named_scope("gather_b1"):
        lax.fori_loop(2, KS, step_b, 0)
    swap(1).start()
    with jax.named_scope("begin_0"):
        rhs = rhs_ref[...]
        state = (jnp.zeros_like(rhs), rhs, rhs, total_of(rhs * rhs))
        early_begin(0, state)
    with jax.named_scope("near_a"):
        near_done(0)
    start(far(0))
    with jax.named_scope("swap_b"):
        combine(1)
    start(near(1))
    with jax.named_scope("near_b"):
        near_done(1)
    start(far(1))
    with jax.named_scope("middle_0"):
        early_middle(0)
    with jax.named_scope("far_a"):
        far_done(0)
    start(spread(0))
    with jax.named_scope("end_0"):
        state = early_end(0, state)
        early_begin(1, state)
    with jax.named_scope("far_b"):
        far_done(1)
    start(spread(1))
    with jax.named_scope("spread_a"):
        wait_recv(spread(0))
    start(share(0))
    with jax.named_scope("middle_1"):
        early_middle(1)
    with jax.named_scope("spread_b"):
        wait_recv(spread(1))
    start(share(1))
    with jax.named_scope("end_1"):
        state = early_end(1, state)
    with jax.named_scope("share_ab"):
        wait_recv(share(0))
        wait_recv(share(1))

    def tile_at(idx):
        return idx // 8, lax.rem(idx, 8) // 2, 2 * lax.rem(idx, 2)

    rel = lax.rem(m + SIDE - y, SIDE)
    out_row = jnp.where(rel == 2, 3, jnp.where(rel == 3, 2, rel))
    giver = x == q

    def out_tile(pc):
        idx = INDEX[0, pc]
        for pr in (1, 2, 3):
            idx = jnp.where(out_row == pr, INDEX[pr, pc], idx)
        return tile_at(idx)

    def give(pc):
        w, qq, mm = out_tile(pc)
        dev = at(xs[REL[pc]], y, z, c)
        return remote(block.at[w, qq, pl.ds(mm, 2)], out_block, o_send.at[pc - 1], o_recv, dev)

    for it in range(EARLY, ITERS):
        with jax.named_scope(f"cg{it}"):
            lines = share_of(state[2], lambda i, p: block[i // 8, (i % 8) // 2, 2 * (i % 2) + p], range(2))
            write_lines(msg, it, lines)
            tell(it)
            if it == ITERS - 1:

                @pl.when(giver)
                def _():
                    for pc in (1, 2, 3):
                        give(pc).start()
                    w, qq, mm = out_tile(0)
                    out_block[...] = block[w, qq, pl.ds(mm, 2)]

            state = update(it, state, heard(it))
    answer = state[0]
    sol_ref[...] = answer

    with jax.named_scope("finish"):

        @pl.when(jnp.logical_not(giver))
        def _():
            give(1).wait_recv()

        for s in range(2):
            schur_ref[SUB * s : SUB * s + SUB] = out_block[s]

        def drain(k, carry):
            for copy in own(k) + onward(k):
                copy.wait_send()
            return carry

        lax.fori_loop(0, KS, drain, 0)
        for w in range(2):
            swap(w).wait_send()
            for copy in near(w) + far(w) + spread(w) + share(w):
                copy.wait_send()
        for it in range(ITERS):
            pltpu.make_async_copy(tally, tally, m_send.at[it]).wait()
        for it in range(EARLY):
            pltpu.make_async_copy(deep_tally, deep_tally, z_send.at[it]).wait()

        @pl.when(giver)
        def _():
            for pc in (1, 2, 3):
                give(pc).wait_send()


def on_device(borders, row_scale, assign, prob, pattern, first_diag, rhs):
    held = pl.BlockSpec(memory_space=pltpu.HBM)
    vmem = pl.BlockSpec(memory_space=pltpu.VMEM)
    dma = pltpu.SemaphoreType.DMA
    schur, answer = pl.pallas_call(
        kernel,
        out_shape=(
            jax.ShapeDtypeStruct((2 * SUB, T), F32),
            jax.ShapeDtypeStruct((SIDE, SIDE, T), F32),
        ),
        in_specs=[held] * 7,
        out_specs=(vmem, vmem),
        scratch_shapes=[
            pltpu.VMEM((1, KS), jnp.int32),
            pltpu.VMEM((1, SCEN), F32),
            pltpu.VMEM((16, SCEN), jnp.int32),
            pltpu.VMEM((KS, R), F32),
            pltpu.VMEM((SIDE, SIDE, T), F32),
            pltpu.VMEM((SIDE, SIDE, T), F32),
            pltpu.VMEM((4, KS, R, T), BF16),
            pltpu.VMEM((4, KS, R, T), BF16),
            pltpu.VMEM((KS, R, NEAR * T), BF16),
            pltpu.VMEM((KS, R, NEAR * T), BF16),
            pltpu.VMEM((KS, R, T), F32),
            pltpu.VMEM((KS, 16, T), F32),
            pltpu.VMEM((16, 2, 2, SUB, T), F32),
            pltpu.VMEM((16, 2, SUB, T), F32),
            pltpu.VMEM((2, 4, 4, SUB, T), F32),
            pltpu.VMEM((2, 3, 4, SUB, T), F32),
            pltpu.VMEM((2, 4, SUB, T), F32),
            pltpu.VMEM((2, 3, SUB, T), F32),
            pltpu.VMEM((2, SUB, T), F32),
            pltpu.VMEM((2, 4, 4, SUB, T), F32),
            pltpu.VMEM((2, SUB, T), F32),
            pltpu.VMEM((SIDE, SIDE, T), F32),
            pltpu.VMEM((ITERS, SIDE, T), F32),
            pltpu.VMEM((ITERS, 8, SIDE, SIDE, T), F32),
            pltpu.VMEM((EARLY, SIDE, T), F32),
            pltpu.VMEM((EARLY, DEPTH, SIDE, T), F32),
            pltpu.VMEM((31, SIDE, T), F32),
            dma((8,)),
            dma((8, KS)),
            dma((8, KS)),
            dma((2,)),
            dma((2,)),
            dma((2, 4)),
            dma((2, 4)),
            dma((2, 3)),
            dma((2, 3)),
            dma((2, 3)),
            dma((2, 3)),
            dma((2, 4)),
            dma((2, 4)),
            dma((3,)),
            dma,
            dma((ITERS,)),
            dma((ITERS,)),
            dma((EARLY,)),
            dma((EARLY,)),
        ],
        compiler_params=pltpu.CompilerParams(
            collective_id=0, has_side_effects=True, vmem_limit_bytes=67_043_328
        ),
    )(
        assign.reshape(1, KS),
        prob.reshape(1, SCEN),
        pattern.T,
        borders,
        row_scale,
        first_diag.reshape(SIDE, SIDE, T),
        rhs.reshape(SIDE, SIDE, T),
    )
    return schur, answer.reshape(SIDE * SIDE * T)


def solution(mesh):
    placed = (P("scen", None, "grp"), P("scen", None), P("scen"), P(), P(), P(), P())
    return jax.shard_map(
        on_device, mesh=mesh, in_specs=placed, out_specs=(P("scen", "grp"), P()), check_vma=False
    )
```

```python
import jax
import jax.numpy as jnp
from jax import lax
from jax.experimental import pallas as pl
from jax.experimental.pallas import tpu as pltpu
from jax.sharding import PartitionSpec as P


ITERS = 5
EARLY = 2
SIDE = 4
DEPTH = 16
SCEN = 192
KS = 6
R = 512
T = 128
HALF = R // 2
PARTS = 8
EACH = 16 // PARTS
SUB = 8
REL = (0, 1, 3, 2)
NEAR = 3
ORDER = [(0, 0), (0, 1), (0, 2), (1, 0), (1, 1), (1, 2), (2, 0), (2, 1)]
ORDER += [(2, 2), (0, 3), (1, 3), (2, 3), (3, 0), (3, 1), (3, 2), (3, 3)]
INDEX = {where: i for i, where in enumerate(ORDER)}
MESH = pl.DeviceIdType.MESH
F32 = jnp.float32
BF16 = jnp.bfloat16


def kernel(
    assign_hbm,
    prob_hbm,
    pattern_hbm,
    b_hbm,
    rs_hbm,
    fd_hbm,
    rhs_hbm,
    schur_hbm,
    sol_hbm,
    assign_ref,
    prob_ref,
    pattern_ref,
    rs_ref,
    fd_ref,
    rhs_ref,
    rowbuf,
    colbuf,
    lefts,
    rights,
    fac,
    pat,
    acc,
    core_in,
    part,
    near_in,
    near_sum,
    far_in,
    mine,
    block,
    out_block,
    dvec,
    msg,
    inbox,
    zmsg,
    zbox,
    tally,
    in_sem,
    g_send,
    g_recv,
    c_send,
    c_recv,
    na_send,
    na_recv,
    fa_send,
    fa_recv,
    fb_send,
    fb_recv,
    nb_send,
    nb_recv,
    o_send,
    o_recv,
    m_send,
    m_recv,
    z_send,
    z_recv,
):
    scen = lax.axis_index("scen")
    grp = lax.axis_index("grp")
    z = scen // 2
    c = lax.rem(scen, 2)
    x = grp // SIDE
    y = lax.rem(grp, SIDE)

    def at(xx, yy, zz, cc):
        return (2 * zz + cc, SIDE * xx + yy)

    def up(v, by, n):
        return lax.rem(v + by, n)

    def remote(src, dst, send, recv, dev):
        return pltpu.make_async_remote_copy(
            src_ref=src, dst_ref=dst, send_sem=send, recv_sem=recv, device_id=dev, device_id_type=MESH
        )

    def landed(like, sem):
        pltpu.make_async_copy(like, like, sem).wait()

    fetch_tiles = tuple(pltpu.make_async_copy(b_hbm.at[k], colbuf.at[0, k], in_sem.at[k]) for k in range(KS))
    fetch_small = tuple(
        pltpu.make_async_copy(src, dst, in_sem.at[KS + i])
        for i, (src, dst) in enumerate(
            (
                (assign_hbm, assign_ref),
                (prob_hbm, prob_ref),
                (pattern_hbm, pattern_ref),
                (rs_hbm, rs_ref),
                (fd_hbm, fd_ref),
                (rhs_hbm, rhs_ref),
                (b_hbm, rowbuf.at[0]),
            )
        )
    )
    for copy in fetch_tiles + fetch_small:
        copy.start()

    xs = [x] + [up(x, by, SIDE) for by in (1, 2, 3)]
    ys = [y] + [up(y, by, SIDE) for by in (1, 2, 3)]
    far_first = sorted(((a, b) for a in range(4) for b in range(4)), key=lambda d: -(min(d[0], 4 - d[0]) + min(d[1], 4 - d[1])))
    plane = []
    for dx, dy in far_first:
        for cc in (c, 1 - c):
            if (dx, dy) != (0, 0) or cc is not c:
                plane.append(at(xs[dx], ys[dy], z, cc))
    deep = {by: at(x, y, up(z, by, DEPTH), c) for by in range(1, DEPTH)}

    with jax.named_scope("entry"):
        barrier = pltpu.get_barrier_semaphore()
        for peer in plane + list(deep.values()):
            pl.semaphore_signal(barrier, inc=1, device_id=peer, device_id_type=MESH)
        pl.semaphore_wait(barrier, len(plane) + len(deep))

    x_next, x_prev, y_next, y_prev = at(xs[1], y, z, c), at(xs[3], y, z, c), at(x, ys[1], z, c), at(x, ys[3], z, c)
    lo, hi = pl.ds(0, HALF), pl.ds(HALF, HALF)

    def hop(buf, kind, src, dst, k, rows, dev):
        return remote(buf.at[src, k, rows], buf.at[dst, k, rows], g_send.at[kind], g_recv.at[kind, k], dev)

    every = pl.ds(0, R)

    def own(k):
        return (
            hop(colbuf, 0, 0, 2, k, every, x_next),
            hop(colbuf, 0, 0, 1, k, every, x_prev),
            remote(colbuf.at[0, k], rowbuf.at[2, k], g_send.at[0], g_recv.at[0, k], y_next),
            remote(colbuf.at[0, k], rowbuf.at[1, k], g_send.at[0], g_recv.at[0, k], y_prev),
        )

    def onward(k):
        return (
            hop(colbuf, 1, 2, 3, k, lo, x_next),
            hop(colbuf, 1, 1, 3, k, hi, x_prev),
            hop(rowbuf, 1, 2, 3, k, lo, y_next),
            hop(rowbuf, 1, 1, 3, k, hi, y_prev),
        )

    for k in range(KS):
        fetch_tiles[k].wait()
        for copy in own(k):
            copy.start()

    with jax.named_scope("setup"):
        for copy in fetch_small:
            copy.wait()
        across = jnp.transpose(jnp.concatenate([rs_ref[...], jnp.zeros((2, R), F32)], axis=0))
        slots = lax.broadcasted_iota(jnp.int32, (1, SCEN), 1)
        present = pattern_ref[...].astype(F32)
        for k in range(KS):
            held = (slots == assign_ref[:, k : k + 1]).astype(F32)
            weight = jnp.sum(prob_ref[...] * held, axis=1, keepdims=True) / SCEN
            fac[k] = jnp.broadcast_to(across[:, k : k + 1] * weight, (R, T))
            pat[k] = jnp.broadcast_to(jnp.sum(present * held, axis=1, keepdims=True), (16, T))
        acc[...] = jnp.zeros_like(acc)

    def masked(p, k):
        keep = pat[k, pl.ds(SIDE * x + ys[REL[p]], 1), :].astype(BF16)
        return rowbuf[p, k] * keep

    def scaled(p, k):
        keep = pat[k, pl.ds(SIDE * xs[REL[p]] + y, 1), :]
        return (colbuf[p, k].astype(F32) * keep * fac[k]).astype(BF16)

    def product(left, right):
        return lax.dot_general(left, right, (((0,), (0,)), ((), ())), preferred_element_type=F32)

    def gain(value, rows, cols):
        for i, pr in enumerate(rows):
            for j, pc in enumerate(cols):
                for h in range(2):
                    for s in range(8):
                        r0 = T * i + 64 * h + SUB * s
                        acc[INDEX[pr, pc], h, s] += value[r0 : r0 + SUB, T * j : T * j + T]

    def step_a(k, carry):
        landed(colbuf.at[:, k], g_recv.at[0, k])
        for copy in onward(k):
            copy.start()
        for p in range(NEAR):
            lefts[k, :, T * p : T * p + T] = masked(p, k)
            rights[k, :, T * p : T * p + T] = scaled(p, k)
        gain(product(lefts[k], rights[k]), range(NEAR), range(NEAR))
        return carry

    def step_b(k, carry):
        landed(colbuf.at[pl.ds(0, 2), k], g_recv.at[1, k])
        left, right = masked(3, k), scaled(3, k)
        gain(product(left, jnp.concatenate([rights[k], right], axis=1)), (3,), range(4))
        gain(product(lefts[k], right), range(NEAR), (3,))
        return carry

    m = lax.rem(z, 4)
    q = z // 4
    ms = [m] + [up(m, by, 4) for by in (1, 2, 3)]
    qs = [q] + [up(q, by, 4) for by in (1, 2, 3)]
    front, back = pl.ds(0, 2), pl.ds(2, 2)

    def swap(w):
        tiles = pl.ds(EACH * w, EACH)
        return remote(acc.at[tiles, 1 - c], core_in.at[tiles], c_send, c_recv.at[w], at(x, y, z, 1 - c))

    def combine(w):
        swap(w).wait_recv()
        for i in range(4):
            tile, s = EACH * w + i // 2, pl.ds(4 * (i % 2), 4)
            part[w, i] = acc[tile, c, s] + core_in[tile, s]

    def near(w):
        return (
            remote(part.at[w, :, ms[1]], near_in.at[w, 0], na_send, na_recv.at[w], deep[1]),
            remote(part.at[w, :, ms[3]], near_in.at[w, 1], na_send, na_recv.at[w], deep[15]),
            remote(part.at[w, front, ms[2]], near_in.at[w, 2, front], na_send, na_recv.at[w], deep[2]),
            remote(part.at[w, back, ms[2]], near_in.at[w, 2, back], na_send, na_recv.at[w], deep[14]),
        )

    def near_done(w):
        landed(near_in.at[w], na_recv.at[w])
        near_sum[w] = part[w, :, m] + near_in[w, 0] + near_in[w, 1] + near_in[w, 2]

    def far(w):
        return tuple(
            remote(near_sum.at[w, qs[s]], far_in.at[w, s - 1], fa_send, fa_recv.at[w], deep[4 * s]) for s in (1, 2, 3)
        )

    def far_done(w):
        landed(far_in.at[w], fa_recv.at[w])
        total = near_sum[w, q] + far_in[w, 0] + far_in[w, 1] + far_in[w, 2]
        if w == 0:
            lane = lax.broadcasted_iota(jnp.int32, (SUB, T), 1)
            row = lax.broadcasted_iota(jnp.int32, (SUB, T), 0)
            diag = jnp.broadcast_to(fd_ref[x, pl.ds(y, 1), :], (SUB, T))
            spot = jnp.where(z < 8, row + 64 * c + SUB * z, -1)
            total = total + jnp.where(lane == spot, diag, 0.0)
        mine[w] = total
        block[w, q, m] = total

    def spread(w):
        return tuple(remote(mine.at[w], block.at[w, q, m], fb_send, fb_recv.at[w], deep[4 * s]) for s in (1, 2, 3))

    def share(w):
        return tuple(
            remote(block.at[w, sel, m], block.at[w, sel, m], nb_send, nb_recv.at[w], deep[by])
            for sel, by in ((pl.ds(0, 4), 1), (pl.ds(0, 4), 15), (front, 2), (back, 14))
        )

    def start(copies):
        for copy in copies:
            copy.start()

    def total_of(v):
        return jnp.sum(jnp.sum(jnp.sum(v, axis=0, keepdims=True), axis=1, keepdims=True), axis=2, keepdims=True)

    def share_of(direction, tile, pieces):
        dvec[...] = direction
        lines = []
        for pr in range(4):
            stack = []
            for piece in pieces:
                prod = None
                for pc in range(4):
                    term = tile(INDEX[pr, pc], piece) * dvec[xs[REL[pc]], pl.ds(y, 1), :]
                    prod = term if prod is None else prod + term
                stack.append(prod)
            both = jnp.concatenate(stack, axis=0)
            if len(pieces) == 8:
                both = jnp.concatenate([jnp.where(c == h, both, jnp.zeros_like(both)) for h in range(2)], axis=0)
            lines.append(jnp.sum(jnp.transpose(both), axis=0, keepdims=True))
        return lines

    def write_lines(ref, it, lines):
        for pr in range(4):
            ref[it, pl.ds(ys[REL[pr]], 1), :] = lines[pr]

    def tell(it):
        for peer in plane:
            remote(msg.at[it], inbox.at[it, 2 * y + c, x], m_send.at[it], m_recv.at[it], peer).start()
        inbox[it, 2 * y + c, x] = msg[it]

    def heard(it):
        landed(tally, m_recv.at[it])
        image = inbox[it, 0]
        for i in range(1, 8):
            image = image + inbox[it, i]
        return image

    deep_tally = tally.at[pl.ds(0, DEPTH - 1)]

    def early_begin(it, state):
        lines = share_of(state[2], lambda i, p: acc[i, p // 8, p % 8], range(16))
        write_lines(zmsg, it, lines)
        for by in (8, 7, 9, 6, 10, 5, 11, 4, 12, 3, 13, 2, 14, 1, 15):
            remote(zmsg.at[it], zbox.at[it, z], z_send.at[it], z_recv.at[it], deep[by]).start()
        zbox[it, z] = zmsg[it]

    def early_middle(it):
        landed(deep_tally, z_recv.at[it])
        total = zbox[it, 0]
        for i in range(1, DEPTH):
            total = total + zbox[it, i]
        msg[it] = total
        tell(it)

    def update(it, state, image):
        answer, residual, direction, norm_now = state
        alpha = norm_now / total_of(direction * image)
        answer = answer + alpha * direction
        if it == ITERS - 1:
            return answer, residual, direction, norm_now
        residual = residual - alpha * image
        norm_next = total_of(residual * residual)
        return answer, residual, residual + (norm_next / norm_now) * direction, norm_next

    def early_end(it, state):
        return update(it, state, heard(it) + fd_ref[...] * state[2])

    early, late = range(PARTS // 2), range(PARTS // 2, PARTS)
    with jax.named_scope("gather_a"):
        lax.fori_loop(0, KS, step_a, 0)
    for w in early:
        swap(w).start()
    with jax.named_scope("gather_b0"):
        lax.fori_loop(0, 1, step_b, 0)
    with jax.named_scope("swap_a"):
        for w in early:
            combine(w)
            start(near(w))
    with jax.named_scope("gather_b1"):
        lax.fori_loop(1, 4, step_b, 0)
    with jax.named_scope("near_a0"):
        for w in early[:2]:
            near_done(w)
            start(far(w))
    with jax.named_scope("gather_b2"):
        lax.fori_loop(4, 5, step_b, 0)
    with jax.named_scope("near_a1"):
        for w in early[2:]:
            near_done(w)
            start(far(w))
    with jax.named_scope("gather_b3"):
        lax.fori_loop(5, KS, step_b, 0)
    for w in late:
        swap(w).start()
    with jax.named_scope("begin_0"):
        rhs = rhs_ref[...]
        state = (jnp.zeros_like(rhs), rhs, rhs, total_of(rhs * rhs))
        early_begin(0, state)
    with jax.named_scope("swap_b"):
        for w in late:
            combine(w)
            start(near(w))
    with jax.named_scope("middle_0"):
        early_middle(0)
    with jax.named_scope("near_b"):
        for w in late:
            near_done(w)
            start(far(w))
    with jax.named_scope("far_a"):
        for w in early:
            far_done(w)
            start(spread(w))
    with jax.named_scope("end_0"):
        state = early_end(0, state)
        early_begin(1, state)
    with jax.named_scope("far_b"):
        for w in late:
            far_done(w)
            start(spread(w))
    with jax.named_scope("spread_a"):
        for w in early:
            landed(far_in.at[w], fb_recv.at[w])
            start(share(w))
    with jax.named_scope("middle_1"):
        early_middle(1)
    with jax.named_scope("spread_b"):
        for w in late:
            landed(far_in.at[w], fb_recv.at[w])
            start(share(w))
    with jax.named_scope("end_1"):
        state = early_end(1, state)
    with jax.named_scope("share_all"):
        for w in range(PARTS):
            landed(near_in.at[w], nb_recv.at[w])

    rel = lax.rem(m + SIDE - y, SIDE)
    out_row = jnp.where(rel == 2, 3, jnp.where(rel == 3, 2, rel))
    giver = x == q
    store_schur = pltpu.make_async_copy(out_block, schur_hbm, in_sem.at[0])
    store_answer = pltpu.make_async_copy(dvec, sol_hbm, in_sem.at[1])

    def out_tile(pc):
        idx = INDEX[0, pc]
        for pr in (1, 2, 3):
            idx = jnp.where(out_row == pr, INDEX[pr, pc], idx)
        return idx // EACH, pl.ds(2 * lax.rem(idx, EACH), 2)

    def give(pc):
        w, t = out_tile(pc)
        dev = at(xs[REL[pc]], y, z, c)
        return remote(block.at[w, t], out_block, o_send, o_recv, dev)

    for it in range(EARLY, ITERS):
        with jax.named_scope(f"cg{it}"):
            lines = share_of(state[2], lambda i, p: block[i // 2, 2 * (i % 2) + p // 4, p % 4], range(8))
            write_lines(msg, it, lines)
            tell(it)
            if it == ITERS - 1:

                @pl.when(giver)
                def _():
                    for pc in (1, 2, 3):
                        give(pc).start()
                    w, t = out_tile(0)
                    out_block[...] = block[w, t]


                @pl.when(jnp.logical_not(giver))
                def _():
                    give(1).wait_recv()

                store_schur.start()
            state = update(it, state, heard(it))
    dvec[...] = state[0]
    store_answer.start()

    with jax.named_scope("finish"):
        landed(colbuf, g_send.at[0])
        landed(colbuf.at[pl.ds(0, 2)], g_send.at[1])
        landed(core_in, c_send)
        landed(near_in, na_send)
        landed(far_in, fa_send)
        landed(far_in, fb_send)
        landed(near_in, nb_send)
        for it in range(ITERS):
            landed(tally, m_send.at[it])
        for it in range(EARLY):
            landed(deep_tally, z_send.at[it])

        @pl.when(giver)
        def _():
            landed(near_in.at[pl.ds(0, 2)], o_send)

        store_schur.wait()
        store_answer.wait()


def on_device(borders, row_scale, assign, prob, pattern, first_diag, rhs):
    held = pl.BlockSpec(memory_space=pltpu.HBM)
    dma = pltpu.SemaphoreType.DMA
    schur, answer = pl.pallas_call(
        kernel,
        out_shape=(
            jax.ShapeDtypeStruct((2, 4, SUB, T), F32),
            jax.ShapeDtypeStruct((SIDE, SIDE, T), F32),
        ),
        in_specs=[held] * 7,
        out_specs=(held, held),
        scratch_shapes=[
            pltpu.VMEM((1, KS), jnp.int32),
            pltpu.VMEM((1, SCEN), F32),
            pltpu.VMEM((16, SCEN), jnp.int32),
            pltpu.VMEM((KS, R), F32),
            pltpu.VMEM((SIDE, SIDE, T), F32),
            pltpu.VMEM((SIDE, SIDE, T), F32),
            pltpu.VMEM((4, KS, R, T), BF16),
            pltpu.VMEM((4, KS, R, T), BF16),
            pltpu.VMEM((KS, R, NEAR * T), BF16),
            pltpu.VMEM((KS, R, NEAR * T), BF16),
            pltpu.VMEM((KS, R, T), F32),
            pltpu.VMEM((KS, 16, T), F32),
            pltpu.VMEM((16, 2, 8, SUB, T), F32),
            pltpu.VMEM((16, 8, SUB, T), F32),
            pltpu.VMEM((PARTS, 4, 4, SUB, T), F32),
            pltpu.VMEM((PARTS, 3, 4, SUB, T), F32),
            pltpu.VMEM((PARTS, 4, SUB, T), F32),
            pltpu.VMEM((PARTS, 3, SUB, T), F32),
            pltpu.VMEM((PARTS, SUB, T), F32),
            pltpu.VMEM((PARTS, 4, 4, SUB, T), F32),
            pltpu.VMEM((2, 4, SUB, T), F32),
            pltpu.VMEM((SIDE, SIDE, T), F32),
            pltpu.VMEM((ITERS, SIDE, T), F32),
            pltpu.VMEM((ITERS, 8, SIDE, SIDE, T), F32),
            pltpu.VMEM((EARLY, SIDE, T), F32),
            pltpu.VMEM((EARLY, DEPTH, SIDE, T), F32),
            pltpu.VMEM((31, SIDE, T), F32),
            dma((KS + 7,)),
            dma((2,)),
            dma((2, KS)),
            dma,
            dma((PARTS,)),
            dma,
            dma((PARTS,)),
            dma,
            dma((PARTS,)),
            dma,
            dma((PARTS,)),
            dma,
            dma((PARTS,)),
            dma,
            dma,
            dma((ITERS,)),
            dma((ITERS,)),
            dma((EARLY,)),
            dma((EARLY,)),
        ],
        compiler_params=pltpu.CompilerParams(
            collective_id=0, has_side_effects=True, vmem_limit_bytes=67_043_328
        ),
    )(
        assign.reshape(1, KS),
        prob.reshape(1, SCEN),
        pattern.T,
        borders,
        row_scale,
        first_diag.reshape(SIDE, SIDE, T),
        rhs.reshape(SIDE, SIDE, T),
    )
    return schur.reshape(8 * SUB, T), answer.reshape(SIDE * SIDE * T)


def solution(mesh):
    placed = (P("scen", None, "grp"), P("scen", None), P("scen"), P(), P(), P(), P())
    return jax.shard_map(
        on_device, mesh=mesh, in_specs=placed, out_specs=(P("scen", "grp"), P()), check_vma=False
    )
```

```python
import jax
import jax.numpy as jnp
from jax import lax
from jax.experimental import pallas as pl
from jax.experimental.pallas import tpu as pltpu
from jax.sharding import PartitionSpec as P


ITERS = 5
EARLY = 2
SIDE = 4
DEPTH = 16
SCEN = 192
KS = 6
R = 512
T = 128
HALF = R // 2
PARTS = 8
EACH = 16 // PARTS
SUB = 8
REL = (0, 1, 3, 2)
NEAR = 3
ORDER = [(0, 0), (0, 1), (0, 2), (1, 0), (1, 1), (1, 2), (2, 0), (2, 1)]
ORDER += [(2, 2), (0, 3), (1, 3), (2, 3), (3, 0), (3, 1), (3, 2), (3, 3)]
INDEX = {where: i for i, where in enumerate(ORDER)}
MESH = pl.DeviceIdType.MESH
F32 = jnp.float32
BF16 = jnp.bfloat16


def kernel(
    assign_hbm,
    prob_hbm,
    pattern_hbm,
    b_hbm,
    rs_hbm,
    fd_hbm,
    rhs_hbm,
    out_hbm,
    assign_ref,
    prob_ref,
    pattern_ref,
    rs_ref,
    fd_ref,
    rhs_ref,
    rowbuf,
    colbuf,
    lefts,
    rights,
    fac,
    pat,
    acc,
    core_in,
    part,
    near_in,
    near_sum,
    far_in,
    mine,
    block,
    out_block,
    final,
    dvec,
    msg,
    inbox,
    zmsg,
    zbox,
    tally,
    in_sem,
    g_send,
    g_recv,
    c_send,
    c_recv,
    na_send,
    na_recv,
    fa_send,
    fa_recv,
    fb_send,
    fb_recv,
    nb_send,
    nb_recv,
    o_send,
    o_recv,
    m_send,
    m_recv,
    z_send,
    z_recv,
    present_sem,
):
    scen = lax.axis_index("scen")
    grp = lax.axis_index("grp")
    z = scen // 2
    c = lax.rem(scen, 2)
    x = grp // SIDE
    y = lax.rem(grp, SIDE)

    def at(xx, yy, zz, cc):
        return (2 * zz + cc, SIDE * xx + yy)

    def up(v, by, n):
        return lax.rem(v + by, n)

    def remote(src, dst, send, recv, dev):
        return pltpu.make_async_remote_copy(
            src_ref=src, dst_ref=dst, send_sem=send, recv_sem=recv, device_id=dev, device_id_type=MESH
        )

    def landed(like, sem):
        pltpu.make_async_copy(like, like, sem).wait()

    fetch_tiles = tuple(pltpu.make_async_copy(b_hbm.at[k], colbuf.at[0, k], in_sem.at[k]) for k in range(KS))
    fetch_small = tuple(
        pltpu.make_async_copy(src, dst, in_sem.at[KS + i])
        for i, (src, dst) in enumerate(
            (
                (assign_hbm, assign_ref),
                (prob_hbm, prob_ref),
                (pattern_hbm, pattern_ref),
                (rs_hbm, rs_ref),
                (fd_hbm, fd_ref),
                (rhs_hbm, rhs_ref),
                (b_hbm, rowbuf.at[0]),
            )
        )
    )
    xs = [x] + [up(x, by, SIDE) for by in (1, 2, 3)]
    ys = [y] + [up(y, by, SIDE) for by in (1, 2, 3)]
    far_first = sorted(((a, b) for a in range(4) for b in range(4)), key=lambda d: -(min(d[0], 4 - d[0]) + min(d[1], 4 - d[1])))
    plane = []
    for dx, dy in far_first:
        for cc in (c, 1 - c):
            if (dx, dy) != (0, 0) or cc is not c:
                plane.append(at(xs[dx], ys[dy], z, cc))
    deep = {by: at(x, y, up(z, by, DEPTH), c) for by in range(1, DEPTH)}

    with jax.named_scope("entry"):
        barrier = pltpu.get_barrier_semaphore()
        first = plane + [deep[by] for by in (1, 2, 14, 15)]
        for peer in first:
            pl.semaphore_signal(barrier, inc=1, device_id=peer, device_id_type=MESH)
        for copy in fetch_tiles + fetch_small:
            copy.start()
        pl.semaphore_wait(barrier, len(first))

    x_next, x_prev, y_next, y_prev = at(xs[1], y, z, c), at(xs[3], y, z, c), at(x, ys[1], z, c), at(x, ys[3], z, c)
    lo, hi = pl.ds(0, HALF), pl.ds(HALF, HALF)

    def hop(buf, kind, src, dst, k, rows, dev):
        return remote(buf.at[src, k, rows], buf.at[dst, k, rows], g_send.at[kind], g_recv.at[kind, k], dev)

    every = pl.ds(0, R)

    def own(k):
        return (
            hop(colbuf, 0, 0, 2, k, every, x_next),
            hop(colbuf, 0, 0, 1, k, every, x_prev),
            remote(colbuf.at[0, k], rowbuf.at[2, k], g_send.at[0], g_recv.at[0, k], y_next),
            remote(colbuf.at[0, k], rowbuf.at[1, k], g_send.at[0], g_recv.at[0, k], y_prev),
        )

    def onward(k):
        return (
            hop(colbuf, 1, 2, 3, k, lo, x_next),
            hop(colbuf, 1, 1, 3, k, hi, x_prev),
            hop(rowbuf, 1, 2, 3, k, lo, y_next),
            hop(rowbuf, 1, 1, 3, k, hi, y_prev),
        )

    for k in range(KS):
        fetch_tiles[k].wait()
        for copy in own(k):
            copy.start()

    def vouch(turn, by):
        for peer in (deep[by], deep[DEPTH - by]):
            pl.semaphore_signal(present_sem.at[turn], inc=1, device_id=peer, device_id_type=MESH)

    def vouched(turn):
        pl.semaphore_wait(present_sem.at[turn], 2)

    vouch(0, 2)

    with jax.named_scope("setup"):
        for copy in fetch_small:
            copy.wait()
        across = jnp.transpose(jnp.concatenate([rs_ref[...], jnp.zeros((2, R), F32)], axis=0))
        slots = lax.broadcasted_iota(jnp.int32, (1, SCEN), 1)
        present = pattern_ref[...].astype(F32)
        for k in range(KS):
            held = (slots == assign_ref[:, k : k + 1]).astype(F32)
            weight = jnp.sum(prob_ref[...] * held, axis=1, keepdims=True) / SCEN
            fac[k] = jnp.broadcast_to(across[:, k : k + 1] * weight, (R, T))
            pat[k] = jnp.broadcast_to(jnp.sum(present * held, axis=1, keepdims=True), (16, T))
        acc[...] = jnp.zeros_like(acc)

    def masked(p, k):
        keep = pat[k, pl.ds(SIDE * x + ys[REL[p]], 1), :].astype(BF16)
        return rowbuf[p, k] * keep

    def scaled(p, k):
        keep = pat[k, pl.ds(SIDE * xs[REL[p]] + y, 1), :]
        return (colbuf[p, k].astype(F32) * keep * fac[k]).astype(BF16)

    def product(left, right):
        return lax.dot_general(left, right, (((0,), (0,)), ((), ())), preferred_element_type=F32)

    def gain(value, rows, cols):
        for i, pr in enumerate(rows):
            for j, pc in enumerate(cols):
                for h in range(2):
                    for s in range(8):
                        r0 = T * i + 64 * h + SUB * s
                        acc[INDEX[pr, pc], h, s] += value[r0 : r0 + SUB, T * j : T * j + T]

    def step_a(k, carry):
        landed(colbuf.at[:, k], g_recv.at[0, k])
        for copy in onward(k):
            copy.start()
        for p in range(NEAR):
            lefts[k, :, T * p : T * p + T] = masked(p, k)
            rights[k, :, T * p : T * p + T] = scaled(p, k)
        gain(product(lefts[k], rights[k]), range(NEAR), range(NEAR))
        return carry

    def step_b(k, carry):
        landed(colbuf.at[pl.ds(0, 2), k], g_recv.at[1, k])
        left, right = masked(3, k), scaled(3, k)
        gain(product(left, jnp.concatenate([rights[k], right], axis=1)), (3,), range(4))
        gain(product(lefts[k], right), range(NEAR), (3,))
        return carry

    m = lax.rem(z, 4)
    q = z // 4
    ms = [m] + [up(m, by, 4) for by in (1, 2, 3)]
    qs = [q] + [up(q, by, 4) for by in (1, 2, 3)]
    front, back = pl.ds(0, 2), pl.ds(2, 2)

    def swap(w):
        tiles = pl.ds(EACH * w, EACH)
        return remote(acc.at[tiles, 1 - c], core_in.at[tiles], c_send, c_recv.at[w], at(x, y, z, 1 - c))

    def combine(w):
        swap(w).wait_recv()
        for i in range(4):
            tile, s = EACH * w + i // 2, pl.ds(4 * (i % 2), 4)
            part[w, i] = acc[tile, c, s] + core_in[tile, s]

    def near(w):
        return (
            remote(part.at[w, :, ms[1]], near_in.at[w, 0], na_send, na_recv.at[w], deep[1]),
            remote(part.at[w, :, ms[3]], near_in.at[w, 1], na_send, na_recv.at[w], deep[15]),
            remote(part.at[w, front, ms[2]], near_in.at[w, 2, front], na_send, na_recv.at[w], deep[2]),
            remote(part.at[w, back, ms[2]], near_in.at[w, 2, back], na_send, na_recv.at[w], deep[14]),
        )

    def near_done(w):
        landed(near_in.at[w], na_recv.at[w])
        near_sum[w] = part[w, :, m] + near_in[w, 0] + near_in[w, 1] + near_in[w, 2]

    def far(w):
        return tuple(
            remote(near_sum.at[w, qs[s]], far_in.at[w, s - 1], fa_send, fa_recv.at[w], deep[4 * s]) for s in (1, 2, 3)
        )

    def far_done(w):
        landed(far_in.at[w], fa_recv.at[w])
        total = near_sum[w, q] + far_in[w, 0] + far_in[w, 1] + far_in[w, 2]
        if w == 0:
            lane = lax.broadcasted_iota(jnp.int32, (SUB, T), 1)
            row = lax.broadcasted_iota(jnp.int32, (SUB, T), 0)
            diag = jnp.broadcast_to(fd_ref[x, pl.ds(y, 1), :], (SUB, T))
            spot = jnp.where(z < 8, row + 64 * c + SUB * z, -1)
            total = total + jnp.where(lane == spot, diag, 0.0)
        mine[w] = total
        block[w, q, m] = total

    def spread(w):
        return tuple(remote(mine.at[w], block.at[w, q, m], fb_send, fb_recv.at[w], deep[4 * s]) for s in (1, 2, 3))

    def share(w):
        return tuple(
            remote(block.at[w, sel, m], block.at[w, sel, m], nb_send, nb_recv.at[w], deep[by])
            for sel, by in ((pl.ds(0, 4), 1), (pl.ds(0, 4), 15), (front, 2), (back, 14))
        )

    def start(copies):
        for copy in copies:
            copy.start()

    def total_of(v):
        return jnp.sum(jnp.sum(jnp.sum(v, axis=0, keepdims=True), axis=1, keepdims=True), axis=2, keepdims=True)

    def share_of(direction, tile, pieces):
        dvec[...] = direction
        lines = []
        for pr in range(4):
            stack = []
            for piece in pieces:
                prod = None
                for pc in range(4):
                    term = tile(INDEX[pr, pc], piece) * dvec[xs[REL[pc]], pl.ds(y, 1), :]
                    prod = term if prod is None else prod + term
                stack.append(prod)
            both = jnp.concatenate(stack, axis=0)
            if len(pieces) == 8:
                both = jnp.concatenate([jnp.where(c == h, both, jnp.zeros_like(both)) for h in range(2)], axis=0)
            lines.append(jnp.sum(jnp.transpose(both), axis=0, keepdims=True))
        return lines

    def write_lines(ref, it, lines):
        for pr in range(4):
            ref[it, pl.ds(ys[REL[pr]], 1), :] = lines[pr]

    def tell(it):
        for peer in plane:
            remote(msg.at[it], inbox.at[it, 2 * y + c, x], m_send.at[it], m_recv.at[it], peer).start()
        inbox[it, 2 * y + c, x] = msg[it]

    def heard(it):
        landed(tally, m_recv.at[it])
        image = inbox[it, 0]
        for i in range(1, 8):
            image = image + inbox[it, i]
        return image

    deep_tally = tally.at[pl.ds(0, DEPTH - 1)]

    def early_begin(it, state):
        lines = share_of(state[2], lambda i, p: acc[i, p // 8, p % 8], range(16))
        write_lines(zmsg, it, lines)
        for by in (8, 7, 9, 6, 10, 5, 11, 4, 12, 3, 13, 2, 14, 1, 15):
            remote(zmsg.at[it], zbox.at[it, z], z_send.at[it], z_recv.at[it], deep[by]).start()
        zbox[it, z] = zmsg[it]

    def early_middle(it):
        landed(deep_tally, z_recv.at[it])
        total = zbox[it, 0]
        for i in range(1, DEPTH):
            total = total + zbox[it, i]
        msg[it] = total
        tell(it)

    def update(it, state, image):
        answer, residual, direction, norm_now = state
        alpha = norm_now / total_of(direction * image)
        answer = answer + alpha * direction
        if it == ITERS - 1:
            return answer, residual, direction, norm_now
        residual = residual - alpha * image
        norm_next = total_of(residual * residual)
        return answer, residual, residual + (norm_next / norm_now) * direction, norm_next

    def early_end(it, state):
        return update(it, state, heard(it) + fd_ref[...] * state[2])

    early, late = range(PARTS // 2), range(PARTS // 2, PARTS)
    with jax.named_scope("gather_a"):
        lax.fori_loop(0, 2, step_a, 0)
        vouched(0)
        vouch(1, 4)
        lax.fori_loop(2, KS, step_a, 0)
        vouched(1)
    for w in early:
        swap(w).start()
    with jax.named_scope("gather_b0"):
        lax.fori_loop(0, 1, step_b, 0)
    with jax.named_scope("swap_a"):
        for w in early:
            combine(w)
            start(near(w))
    with jax.named_scope("gather_b1"):
        lax.fori_loop(1, 4, step_b, 0)
    with jax.named_scope("near_a0"):
        for w in early[:2]:
            near_done(w)
            start(far(w))
    with jax.named_scope("gather_b2"):
        lax.fori_loop(4, 5, step_b, 0)
    with jax.named_scope("near_a1"):
        for w in early[2:]:
            near_done(w)
            start(far(w))
    with jax.named_scope("gather_b3"):
        lax.fori_loop(5, KS, step_b, 0)
    for w in late:
        swap(w).start()
    with jax.named_scope("begin_0"):
        rhs = rhs_ref[...]
        state = (jnp.zeros_like(rhs), rhs, rhs, total_of(rhs * rhs))
        early_begin(0, state)
    with jax.named_scope("swap_b"):
        for w in late:
            combine(w)
            start(near(w))
    with jax.named_scope("middle_0"):
        early_middle(0)
    with jax.named_scope("near_b"):
        for w in late:
            near_done(w)
            start(far(w))
    with jax.named_scope("far_a"):
        for w in early:
            far_done(w)
            start(spread(w))
    with jax.named_scope("end_0"):
        state = early_end(0, state)
        early_begin(1, state)
    with jax.named_scope("far_b"):
        for w in late:
            far_done(w)
            start(spread(w))
    with jax.named_scope("spread_a"):
        for w in early:
            landed(far_in.at[w], fb_recv.at[w])
            start(share(w))
    with jax.named_scope("middle_1"):
        early_middle(1)
    with jax.named_scope("spread_b"):
        for w in late:
            landed(far_in.at[w], fb_recv.at[w])
            start(share(w))
    with jax.named_scope("end_1"):
        state = early_end(1, state)
    with jax.named_scope("share_all"):
        for w in range(PARTS):
            landed(near_in.at[w], nb_recv.at[w])

    rel = lax.rem(m + SIDE - y, SIDE)
    out_row = jnp.where(rel == 2, 3, jnp.where(rel == 3, 2, rel))
    giver = x == q
    store_schur = tuple(
        pltpu.make_async_copy(out_block.at[i], out_hbm.at[pl.ds(4 * i, 4)], in_sem.at[i]) for i in range(2)
    )
    store_answer = pltpu.make_async_copy(final, out_hbm.at[pl.ds(8, 2)], in_sem.at[2])

    def out_tile(pc):
        idx = INDEX[0, pc]
        for pr in (1, 2, 3):
            idx = jnp.where(out_row == pr, INDEX[pr, pc], idx)
        return idx // EACH, pl.ds(2 * lax.rem(idx, EACH), 2)

    def give(pc):
        w, t = out_tile(pc)
        dev = at(xs[REL[pc]], y, z, c)
        return remote(block.at[w, t], out_block, o_send, o_recv, dev)

    for it in range(EARLY, ITERS):
        with jax.named_scope(f"cg{it}"):
            lines = share_of(state[2], lambda i, p: block[i // 2, 2 * (i % 2) + p // 4, p % 4], range(8))
            write_lines(msg, it, lines)
            tell(it)
            if it == ITERS - 1:

                @pl.when(giver)
                def _():
                    for pc in (1, 2, 3):
                        give(pc).start()
                    w, t = out_tile(0)
                    out_block[...] = block[w, t]


                @pl.when(jnp.logical_not(giver))
                def _():
                    give(1).wait_recv()

                start(store_schur)
            state = update(it, state, heard(it))
    for i in range(SIDE):
        final[i // 2, 4 * (i % 2) : 4 * (i % 2) + 4] = state[0][i]
    store_answer.start()

    with jax.named_scope("finish"):
        landed(colbuf, g_send.at[0])
        landed(colbuf.at[pl.ds(0, 2)], g_send.at[1])
        landed(core_in, c_send)
        landed(near_in, na_send)
        landed(far_in, fa_send)
        landed(far_in, fb_send)
        landed(near_in, nb_send)
        for it in range(ITERS):
            landed(tally, m_send.at[it])
        for it in range(EARLY):
            landed(deep_tally, z_send.at[it])

        @pl.when(giver)
        def _():
            landed(near_in.at[pl.ds(0, 2)], o_send)

        for copy in store_schur + (store_answer,):
            copy.wait()


def on_device(borders, row_scale, assign, prob, pattern, first_diag, rhs):
    held = pl.BlockSpec(memory_space=pltpu.HBM)
    dma = pltpu.SemaphoreType.DMA
    out = pl.pallas_call(
        kernel,
        out_shape=jax.ShapeDtypeStruct((10, 8, T), F32),
        in_specs=[held] * 7,
        out_specs=held,
        scratch_shapes=[
            pltpu.VMEM((1, KS), jnp.int32),
            pltpu.VMEM((1, SCEN), F32),
            pltpu.VMEM((16, SCEN), jnp.int32),
            pltpu.VMEM((KS, R), F32),
            pltpu.VMEM((SIDE, SIDE, T), F32),
            pltpu.VMEM((SIDE, SIDE, T), F32),
            pltpu.VMEM((4, KS, R, T), BF16),
            pltpu.VMEM((4, KS, R, T), BF16),
            pltpu.VMEM((KS, R, NEAR * T), BF16),
            pltpu.VMEM((KS, R, NEAR * T), BF16),
            pltpu.VMEM((KS, R, T), F32),
            pltpu.VMEM((KS, 16, T), F32),
            pltpu.VMEM((16, 2, 8, SUB, T), F32),
            pltpu.VMEM((16, 8, SUB, T), F32),
            pltpu.VMEM((PARTS, 4, 4, SUB, T), F32),
            pltpu.VMEM((PARTS, 3, 4, SUB, T), F32),
            pltpu.VMEM((PARTS, 4, SUB, T), F32),
            pltpu.VMEM((PARTS, 3, SUB, T), F32),
            pltpu.VMEM((PARTS, SUB, T), F32),
            pltpu.VMEM((PARTS, 4, 4, SUB, T), F32),
            pltpu.VMEM((2, 4, SUB, T), F32),
            pltpu.VMEM((2, 8, T), F32),
            pltpu.VMEM((SIDE, SIDE, T), F32),
            pltpu.VMEM((ITERS, SIDE, T), F32),
            pltpu.VMEM((ITERS, 8, SIDE, SIDE, T), F32),
            pltpu.VMEM((EARLY, SIDE, T), F32),
            pltpu.VMEM((EARLY, DEPTH, SIDE, T), F32),
            pltpu.VMEM((31, SIDE, T), F32),
            dma((KS + 7,)),
            dma((2,)),
            dma((2, KS)),
            dma,
            dma((PARTS,)),
            dma,
            dma((PARTS,)),
            dma,
            dma((PARTS,)),
            dma,
            dma((PARTS,)),
            dma,
            dma((PARTS,)),
            dma,
            dma,
            dma((ITERS,)),
            dma((ITERS,)),
            dma((EARLY,)),
            dma((EARLY,)),
            pltpu.SemaphoreType.REGULAR((2,)),
        ],
        compiler_params=pltpu.CompilerParams(
            collective_id=0, has_side_effects=True, vmem_limit_bytes=67_043_328
        ),
    )(
        assign.reshape(1, KS),
        prob.reshape(1, SCEN),
        pattern.T,
        borders,
        row_scale,
        first_diag.reshape(SIDE, SIDE, T),
        rhs.reshape(SIDE, SIDE, T),
    )
    return out[:8].reshape(8 * SUB, T), out[8:].reshape(SIDE * SIDE * T)


def solution(mesh):
    placed = (P("scen", None, "grp"), P("scen", None), P("scen"), P(), P(), P(), P())
    return jax.shard_map(
        on_device, mesh=mesh, in_specs=placed, out_specs=(P("scen", "grp"), P()), check_vma=False
    )
```

```python
import jax
import jax.numpy as jnp
from jax import lax
from jax.experimental import pallas as pl
from jax.experimental.pallas import tpu as pltpu
from jax.sharding import PartitionSpec as P


ITERS = 5
EARLY = 2
SIDE = 4
DEPTH = 16
SCEN = 192
KS = 6
R = 512
T = 128
HALF = R // 2
PARTS = 8
EACH = 16 // PARTS
SUB = 8
REL = (0, 1, 3, 2)
NEAR = 3
ORDER = [(0, 0), (0, 1), (0, 2), (1, 0), (1, 1), (1, 2), (2, 0), (2, 1)]
ORDER += [(2, 2), (0, 3), (1, 3), (2, 3), (3, 0), (3, 1), (3, 2), (3, 3)]
INDEX = {where: i for i, where in enumerate(ORDER)}
MESH = pl.DeviceIdType.MESH
F32 = jnp.float32
BF16 = jnp.bfloat16


def kernel(
    assign_hbm,
    prob_hbm,
    pattern_hbm,
    b_hbm,
    rs_hbm,
    fd_hbm,
    rhs_hbm,
    out_hbm,
    assign_ref,
    prob_ref,
    pattern_ref,
    rs_ref,
    fd_ref,
    rhs_ref,
    rowbuf,
    colbuf,
    lefts,
    rights,
    fac,
    pat,
    acc,
    core_in,
    part,
    near_in,
    near_sum,
    far_in,
    mine,
    block,
    out_block,
    final,
    dvec,
    msg,
    inbox,
    zmsg,
    zbox,
    tally,
    halves,
    msg_half,
    inbox_half,
    tally_half,
    in_sem,
    g_send,
    g_recv,
    c_send,
    c_recv,
    na_send,
    na_recv,
    fa_send,
    fa_recv,
    fb_send,
    fb_recv,
    nb_send,
    nb_recv,
    o_send,
    o_recv,
    m_send,
    m_recv,
    z_send,
    z_recv,
    present_sem,
):
    scen = lax.axis_index("scen")
    grp = lax.axis_index("grp")
    z = scen // 2
    c = lax.rem(scen, 2)
    x = grp // SIDE
    y = lax.rem(grp, SIDE)

    def at(xx, yy, zz, cc):
        return (2 * zz + cc, SIDE * xx + yy)

    def up(v, by, n):
        return lax.rem(v + by, n)

    def remote(src, dst, send, recv, dev):
        return pltpu.make_async_remote_copy(
            src_ref=src, dst_ref=dst, send_sem=send, recv_sem=recv, device_id=dev, device_id_type=MESH
        )

    def landed(like, sem):
        pltpu.make_async_copy(like, like, sem).wait()

    fetch_tiles = tuple(pltpu.make_async_copy(b_hbm.at[k], colbuf.at[0, k], in_sem.at[k]) for k in range(KS))
    fetch_small = tuple(
        pltpu.make_async_copy(src, dst, in_sem.at[KS + i])
        for i, (src, dst) in enumerate(
            (
                (assign_hbm, assign_ref),
                (prob_hbm, prob_ref),
                (pattern_hbm, pattern_ref),
                (rs_hbm, rs_ref),
                (fd_hbm, fd_ref),
                (rhs_hbm, rhs_ref),
                (b_hbm, rowbuf.at[0]),
            )
        )
    )
    xs = [x] + [up(x, by, SIDE) for by in (1, 2, 3)]
    ys = [y] + [up(y, by, SIDE) for by in (1, 2, 3)]
    far_first = sorted(((a, b) for a in range(4) for b in range(4)), key=lambda d: -(min(d[0], 4 - d[0]) + min(d[1], 4 - d[1])))
    plane = []
    for dx, dy in far_first:
        for cc in (c, 1 - c):
            if (dx, dy) != (0, 0) or cc is not c:
                plane.append(at(xs[dx], ys[dy], z, cc))
    deep = {by: at(x, y, up(z, by, DEPTH), c) for by in range(1, DEPTH)}

    ring = [at(xs[1], y, z, c), at(xs[3], y, z, c), at(x, ys[1], z, c), at(x, ys[3], z, c)]

    with jax.named_scope("entry"):
        barrier = pltpu.get_barrier_semaphore()
        first = ring + [at(x, y, z, 1 - c), deep[1], deep[15]]
        for peer in first:
            pl.semaphore_signal(barrier, inc=1, device_id=peer, device_id_type=MESH)
        for copy in fetch_tiles + fetch_small:
            copy.start()
        pl.semaphore_wait(barrier, len(first))

    x_next, x_prev, y_next, y_prev = at(xs[1], y, z, c), at(xs[3], y, z, c), at(x, ys[1], z, c), at(x, ys[3], z, c)
    lo, hi = pl.ds(0, HALF), pl.ds(HALF, HALF)

    def hop(buf, kind, src, dst, k, rows, dev):
        return remote(buf.at[src, k, rows], buf.at[dst, k, rows], g_send.at[kind], g_recv.at[kind, k], dev)

    every = pl.ds(0, R)

    def own(k):
        return (
            hop(colbuf, 0, 0, 2, k, every, x_next),
            hop(colbuf, 0, 0, 1, k, every, x_prev),
            remote(colbuf.at[0, k], rowbuf.at[2, k], g_send.at[0], g_recv.at[0, k], y_next),
            remote(colbuf.at[0, k], rowbuf.at[1, k], g_send.at[0], g_recv.at[0, k], y_prev),
        )

    def onward(k):
        return (
            hop(colbuf, 1, 2, 3, k, lo, x_next),
            hop(colbuf, 1, 1, 3, k, hi, x_prev),
            hop(rowbuf, 1, 2, 3, k, lo, y_next),
            hop(rowbuf, 1, 1, 3, k, hi, y_prev),
        )

    for k in range(KS):
        fetch_tiles[k].wait()
        for copy in own(k):
            copy.start()

    def vouch(turn):
        peers = list(ring)
        if turn < 3:
            peers += [deep[2**turn], deep[DEPTH - 2**turn]]
        for i, peer in enumerate(peers):
            sem = present_sem.at[turn] if i < 4 else present_sem.at[4 + turn]
            pl.semaphore_signal(sem, inc=1, device_id=peer, device_id_type=MESH)

    def vouched(turn):
        pl.semaphore_wait(present_sem.at[turn], 4)
        if turn < 3:
            pl.semaphore_wait(present_sem.at[4 + turn], 2)

    vouch(0)

    with jax.named_scope("setup"):
        for copy in fetch_small:
            copy.wait()
        across = jnp.transpose(jnp.concatenate([rs_ref[...], jnp.zeros((2, R), F32)], axis=0))
        slots = lax.broadcasted_iota(jnp.int32, (1, SCEN), 1)
        present = pattern_ref[...].astype(F32)
        for k in range(KS):
            held = (slots == assign_ref[:, k : k + 1]).astype(F32)
            weight = jnp.sum(prob_ref[...] * held, axis=1, keepdims=True) / SCEN
            fac[k] = jnp.broadcast_to(across[:, k : k + 1] * weight, (R, T))
            pat[k] = jnp.broadcast_to(jnp.sum(present * held, axis=1, keepdims=True), (16, T))
        acc[...] = jnp.zeros_like(acc)

    def masked(p, k):
        keep = pat[k, pl.ds(SIDE * x + ys[REL[p]], 1), :].astype(BF16)
        return rowbuf[p, k] * keep

    def scaled(p, k):
        keep = pat[k, pl.ds(SIDE * xs[REL[p]] + y, 1), :]
        return (colbuf[p, k].astype(F32) * keep * fac[k]).astype(BF16)

    def product(left, right):
        return lax.dot_general(left, right, (((0,), (0,)), ((), ())), preferred_element_type=F32)

    def gain(value, rows, cols):
        for i, pr in enumerate(rows):
            for j, pc in enumerate(cols):
                for h in range(2):
                    for s in range(8):
                        r0 = T * i + 64 * h + SUB * s
                        acc[INDEX[pr, pc], h, s] += value[r0 : r0 + SUB, T * j : T * j + T]

    def step_a(k, carry):
        landed(colbuf.at[:, k], g_recv.at[0, k])
        for copy in onward(k):
            copy.start()
        for p in range(NEAR):
            lefts[k, :, T * p : T * p + T] = masked(p, k)
            rights[k, :, T * p : T * p + T] = scaled(p, k)
        gain(product(lefts[k], rights[k]), range(NEAR), range(NEAR))
        for turn in range(4):

            @pl.when(k == turn + 1)
            def _():
                vouched(turn)
                if turn < 3:
                    vouch(turn + 1)

        return carry

    def step_b(k, carry):
        landed(colbuf.at[pl.ds(0, 2), k], g_recv.at[1, k])
        left, right = masked(3, k), scaled(3, k)
        gain(product(left, jnp.concatenate([rights[k], right], axis=1)), (3,), range(4))
        gain(product(lefts[k], right), range(NEAR), (3,))
        return carry

    m = lax.rem(z, 4)
    q = z // 4
    ms = [m] + [up(m, by, 4) for by in (1, 2, 3)]
    qs = [q] + [up(q, by, 4) for by in (1, 2, 3)]
    front, back = pl.ds(0, 2), pl.ds(2, 2)

    def swap(w):
        tiles = pl.ds(EACH * w, EACH)
        return remote(acc.at[tiles, 1 - c], core_in.at[tiles], c_send, c_recv.at[w], at(x, y, z, 1 - c))

    def combine(w):
        swap(w).wait_recv()
        for i in range(4):
            tile, s = EACH * w + i // 2, pl.ds(4 * (i % 2), 4)
            part[w, i] = acc[tile, c, s] + core_in[tile, s]

    def near(w):
        return (
            remote(part.at[w, :, ms[1]], near_in.at[w, 0], na_send, na_recv.at[w], deep[1]),
            remote(part.at[w, :, ms[3]], near_in.at[w, 1], na_send, na_recv.at[w], deep[15]),
            remote(part.at[w, front, ms[2]], near_in.at[w, 2, front], na_send, na_recv.at[w], deep[2]),
            remote(part.at[w, back, ms[2]], near_in.at[w, 2, back], na_send, na_recv.at[w], deep[14]),
        )

    def near_done(w):
        landed(near_in.at[w], na_recv.at[w])
        near_sum[w] = part[w, :, m] + near_in[w, 0] + near_in[w, 1] + near_in[w, 2]

    def far(w):
        return tuple(
            remote(near_sum.at[w, qs[s]], far_in.at[w, s - 1], fa_send, fa_recv.at[w], deep[4 * s]) for s in (1, 2, 3)
        )

    def far_done(w):
        landed(far_in.at[w], fa_recv.at[w])
        total = near_sum[w, q] + far_in[w, 0] + far_in[w, 1] + far_in[w, 2]
        if w == 0:
            lane = lax.broadcasted_iota(jnp.int32, (SUB, T), 1)
            row = lax.broadcasted_iota(jnp.int32, (SUB, T), 0)
            diag = jnp.broadcast_to(fd_ref[x, pl.ds(y, 1), :], (SUB, T))
            spot = jnp.where(z < 8, row + 64 * c + SUB * z, -1)
            total = total + jnp.where(lane == spot, diag, 0.0)
        mine[w] = total
        block[w, q, m] = total

    def spread(w):
        return tuple(remote(mine.at[w], block.at[w, q, m], fb_send, fb_recv.at[w], deep[4 * s]) for s in (1, 2, 3))

    def share(w):
        return tuple(
            remote(block.at[w, sel, m], block.at[w, sel, m], nb_send, nb_recv.at[w], deep[by])
            for sel, by in ((pl.ds(0, 4), 1), (pl.ds(0, 4), 15), (front, 2), (back, 14))
        )

    def start(copies):
        for copy in copies:
            copy.start()

    def total_of(v):
        for axis in range(v.ndim):
            v = jnp.sum(v, axis=axis, keepdims=True)
        return v

    def share_of(tile, pieces, d_row):
        lines = []
        for pr in range(4):
            stack = []
            for piece in pieces:
                prod = None
                for pc in range(4):
                    term = tile(INDEX[pr, pc], piece) * d_row(xs[REL[pc]])
                    prod = term if prod is None else prod + term
                stack.append(prod)
            both = jnp.concatenate(stack, axis=0)
            if len(pieces) == 8:
                odd = lax.rem(ys[REL[pr]], 2)
                both = jnp.concatenate([jnp.where(odd == h, both, jnp.zeros_like(both)) for h in range(2)], axis=0)
            lines.append(jnp.sum(jnp.transpose(both), axis=0, keepdims=True))
        return lines

    def write_lines(ref, it, lines):
        for pr in range(4):
            ref[it, pl.ds(ys[REL[pr]], 1), :] = lines[pr]

    def tell(it):
        for peer in plane:
            remote(msg.at[it], inbox.at[it, 2 * y + c, x], m_send.at[it], m_recv.at[it], peer).start()
        inbox[it, 2 * y + c, x] = msg[it]

    def heard(it):
        landed(tally, m_recv.at[it])
        image = inbox[it, 0]
        for i in range(1, 8):
            image = image + inbox[it, i]
        return image

    deep_tally = tally.at[pl.ds(0, DEPTH - 1)]

    def early_begin(it, state):
        dvec[...] = state[2]
        lines = share_of(lambda i, p: acc[i, p // 8, p % 8], range(16), lambda xx: dvec[xx, pl.ds(y, 1), :])
        write_lines(zmsg, it, lines)
        for by in (8, 7, 9, 6, 10, 5, 11, 4, 12, 3, 13, 2, 14, 1, 15):
            remote(zmsg.at[it], zbox.at[it, z], z_send.at[it], z_recv.at[it], deep[by]).start()
        zbox[it, z] = zmsg[it]

    def early_middle(it):
        landed(deep_tally, z_recv.at[it])
        total = zbox[it, 0]
        for i in range(1, DEPTH):
            total = total + zbox[it, i]
        msg[it] = total
        tell(it)

    def update(it, state, image):
        answer, residual, direction, norm_now = state
        alpha = norm_now / total_of(direction * image)
        answer = answer + alpha * direction
        if it == ITERS - 1:
            return answer, residual, direction, norm_now
        residual = residual - alpha * image
        norm_next = total_of(residual * residual)
        return answer, residual, residual + (norm_next / norm_now) * direction, norm_next

    def early_end(it, state):
        return update(it, state, heard(it) + fd_ref[...] * state[2])

    early, late = range(PARTS // 2), range(PARTS // 2, PARTS)
    with jax.named_scope("gather_a"):
        lax.fori_loop(0, KS, step_a, 0)
    for w in early:
        swap(w).start()
    with jax.named_scope("gather_b0"):
        lax.fori_loop(0, 1, step_b, 0)
    with jax.named_scope("swap_a"):
        for w in early:
            combine(w)
            start(near(w))
    with jax.named_scope("gather_b1"):
        lax.fori_loop(1, 4, step_b, 0)
    with jax.named_scope("near_a0"):
        for w in early[:2]:
            near_done(w)
            start(far(w))
    with jax.named_scope("gather_b2"):
        lax.fori_loop(4, 5, step_b, 0)
    with jax.named_scope("near_a1"):
        for w in early[2:]:
            near_done(w)
            start(far(w))
    with jax.named_scope("gather_b3"):
        lax.fori_loop(5, KS, step_b, 0)
    for w in late:
        swap(w).start()
    with jax.named_scope("begin_0"):
        rhs = rhs_ref[...]
        state = (jnp.zeros_like(rhs), rhs, rhs, total_of(rhs * rhs))
        early_begin(0, state)
    with jax.named_scope("swap_b"):
        for w in late:
            combine(w)
            start(near(w))
    with jax.named_scope("middle_0"):
        early_middle(0)
    with jax.named_scope("near_b"):
        for w in late:
            near_done(w)
            start(far(w))
    with jax.named_scope("far_a"):
        for w in early:
            far_done(w)
            start(spread(w))
    with jax.named_scope("end_0"):
        state = early_end(0, state)
        early_begin(1, state)
    with jax.named_scope("far_b"):
        for w in late:
            far_done(w)
            start(spread(w))
    with jax.named_scope("spread_a"):
        for w in early:
            landed(far_in.at[w], fb_recv.at[w])
            start(share(w))
    with jax.named_scope("middle_1"):
        early_middle(1)
    with jax.named_scope("spread_b"):
        for w in late:
            landed(far_in.at[w], fb_recv.at[w])
            start(share(w))
    with jax.named_scope("end_1"):
        state = early_end(1, state)
    with jax.named_scope("share_all"):
        for w in range(PARTS):
            landed(near_in.at[w], nb_recv.at[w])

    rel = lax.rem(m + SIDE - y, SIDE)
    out_row = jnp.where(rel == 2, 3, jnp.where(rel == 3, 2, rel))
    giver = x == q
    store_schur = tuple(
        pltpu.make_async_copy(out_block.at[i], out_hbm.at[pl.ds(4 * i, 4)], in_sem.at[i]) for i in range(2)
    )
    store_answer = pltpu.make_async_copy(final, out_hbm.at[pl.ds(8, 2)], in_sem.at[2])

    def out_tile(pc):
        idx = INDEX[0, pc]
        for pr in (1, 2, 3):
            idx = jnp.where(out_row == pr, INDEX[pr, pc], idx)
        return idx // EACH, pl.ds(2 * lax.rem(idx, EACH), 2)

    def give(pc):
        w, t = out_tile(pc)
        dev = at(xs[REL[pc]], y, z, c)
        return remote(block.at[w, t], out_block, o_send, o_recv, dev)

    def split(v):
        for p in range(2):
            for i in range(2):
                halves[p, :, i : i + 1, :] = v[:, 2 * i + p : 2 * i + p + 1, :]
        return halves[...]

    low = lax.broadcasted_iota(jnp.int32, (SIDE, 2, T), 2) < 64

    def heard_halves(n, it):
        landed(tally_half, m_recv.at[it])
        ours = []
        for cc in range(2):
            total = inbox_half[n, cc]
            for i in range(1, SIDE):
                total = total + inbox_half[n, 2 * i + cc]
            ours.append(total)
        turned = [pltpu.roll(v, 64, axis=2) for v in ours]
        return jnp.stack([jnp.where(low, ours[0], turned[1]), jnp.where(low, turned[0], ours[1])])

    state = tuple(split(v) for v in state[:3]) + (state[3].reshape(1, 1, 1, 1),)
    for n, it in enumerate(range(EARLY, ITERS)):
        with jax.named_scope(f"cg{it}"):
            halves[...] = state[2]
            lines = share_of(
                lambda i, p: block[i // 2, 2 * (i % 2) + p // 4, p % 4],
                range(8),
                lambda xx: halves[lax.rem(y, 2), xx, pl.ds(y // 2, 1), :],
            )
            write_lines(msg, it, lines)
            for i in range(2):
                msg_half[n, i : i + 1] = msg[it, 2 * i : 2 * i + 1] + msg[it, 2 * i + 1 : 2 * i + 2]
            for peer in plane:
                remote(msg_half.at[n], inbox_half.at[n, 2 * y + c, x], m_send.at[it], m_recv.at[it], peer).start()
            inbox_half[n, 2 * y + c, x] = msg_half[n]
            if it == ITERS - 1:

                @pl.when(giver)
                def _():
                    for pc in (1, 2, 3):
                        give(pc).start()
                    w, t = out_tile(0)
                    out_block[...] = block[w, t]

                @pl.when(jnp.logical_not(giver))
                def _():
                    give(1).wait_recv()

                start(store_schur)
            state = update(it, state, heard_halves(n, it))
    for xx in range(SIDE):
        for i in range(2):
            for p in range(2):
                row = 4 * (xx % 2) + 2 * i + p
                final[xx // 2, row : row + 1, :] = state[0][p, xx, i : i + 1, :]
    store_answer.start()

    with jax.named_scope("finish"):
        landed(colbuf, g_send.at[0])
        landed(colbuf.at[pl.ds(0, 2)], g_send.at[1])
        landed(core_in, c_send)
        landed(near_in, na_send)
        landed(far_in, fa_send)
        landed(far_in, fb_send)
        landed(near_in, nb_send)
        for it in range(ITERS):
            landed(tally if it < EARLY else tally_half, m_send.at[it])
        for it in range(EARLY):
            landed(deep_tally, z_send.at[it])

        @pl.when(giver)
        def _():
            landed(near_in.at[pl.ds(0, 2)], o_send)

        for copy in store_schur + (store_answer,):
            copy.wait()


def on_device(borders, row_scale, assign, prob, pattern, first_diag, rhs):
    held = pl.BlockSpec(memory_space=pltpu.HBM)
    dma = pltpu.SemaphoreType.DMA
    out = pl.pallas_call(
        kernel,
        out_shape=jax.ShapeDtypeStruct((10, 8, T), F32),
        in_specs=[held] * 7,
        out_specs=held,
        scratch_shapes=[
            pltpu.VMEM((1, KS), jnp.int32),
            pltpu.VMEM((1, SCEN), F32),
            pltpu.VMEM((16, SCEN), jnp.int32),
            pltpu.VMEM((KS, R), F32),
            pltpu.VMEM((SIDE, SIDE, T), F32),
            pltpu.VMEM((SIDE, SIDE, T), F32),
            pltpu.VMEM((4, KS, R, T), BF16),
            pltpu.VMEM((4, KS, R, T), BF16),
            pltpu.VMEM((KS, R, NEAR * T), BF16),
            pltpu.VMEM((KS, R, NEAR * T), BF16),
            pltpu.VMEM((KS, R, T), F32),
            pltpu.VMEM((KS, 16, T), F32),
            pltpu.VMEM((16, 2, 8, SUB, T), F32),
            pltpu.VMEM((16, 8, SUB, T), F32),
            pltpu.VMEM((PARTS, 4, 4, SUB, T), F32),
            pltpu.VMEM((PARTS, 3, 4, SUB, T), F32),
            pltpu.VMEM((PARTS, 4, SUB, T), F32),
            pltpu.VMEM((PARTS, 3, SUB, T), F32),
            pltpu.VMEM((PARTS, SUB, T), F32),
            pltpu.VMEM((PARTS, 4, 4, SUB, T), F32),
            pltpu.VMEM((2, 4, SUB, T), F32),
            pltpu.VMEM((2, 8, T), F32),
            pltpu.VMEM((SIDE, SIDE, T), F32),
            pltpu.VMEM((ITERS, SIDE, T), F32),
            pltpu.VMEM((EARLY, 8, SIDE, SIDE, T), F32),
            pltpu.VMEM((EARLY, SIDE, T), F32),
            pltpu.VMEM((EARLY, DEPTH, SIDE, T), F32),
            pltpu.VMEM((31, SIDE, T), F32),
            pltpu.VMEM((2, SIDE, 2, T), F32),
            pltpu.VMEM((ITERS - EARLY, 2, T), F32),
            pltpu.VMEM((ITERS - EARLY, 8, SIDE, 2, T), F32),
            pltpu.VMEM((31, 2, T), F32),
            dma((KS + 7,)),
            dma((2,)),
            dma((2, KS)),
            dma,
            dma((PARTS,)),
            dma,
            dma((PARTS,)),
            dma,
            dma((PARTS,)),
            dma,
            dma((PARTS,)),
            dma,
            dma((PARTS,)),
            dma,
            dma,
            dma((ITERS,)),
            dma((ITERS,)),
            dma((EARLY,)),
            dma((EARLY,)),
            pltpu.SemaphoreType.REGULAR((7,)),
        ],
        compiler_params=pltpu.CompilerParams(
            collective_id=0, has_side_effects=True, vmem_limit_bytes=67_043_328
        ),
    )(
        assign.reshape(1, KS),
        prob.reshape(1, SCEN),
        pattern.T,
        borders,
        row_scale,
        first_diag.reshape(SIDE, SIDE, T),
        rhs.reshape(SIDE, SIDE, T),
    )
    return out[:8].reshape(8 * SUB, T), out[8:].reshape(SIDE * SIDE * T)


def solution(mesh):
    placed = (P("scen", None, "grp"), P("scen", None), P("scen"), P(), P(), P(), P())
    return jax.shard_map(
        on_device, mesh=mesh, in_specs=placed, out_specs=(P("scen", "grp"), P()), check_vma=False
    )
```

```python
import jax
import jax.numpy as jnp
from jax import lax
from jax.experimental import pallas as pl
from jax.experimental.pallas import tpu as pltpu
from jax.sharding import PartitionSpec as P


ITERS = 5
EARLY = 2
SIDE = 4
DEPTH = 16
SCEN = 192
KS = 6
R = 512
T = 128
HALF = R // 2
PARTS = 8
EACH = 16 // PARTS
SUB = 8
REL = (0, 1, 3, 2)
NEAR = 3
ORDER = [(0, 0), (0, 1), (0, 2), (1, 0), (1, 1), (1, 2), (2, 0), (2, 1)]
ORDER += [(2, 2), (0, 3), (1, 3), (2, 3), (3, 0), (3, 1), (3, 2), (3, 3)]
INDEX = {where: i for i, where in enumerate(ORDER)}
MESH = pl.DeviceIdType.MESH
F32 = jnp.float32
BF16 = jnp.bfloat16


def kernel(
    assign_hbm,
    prob_hbm,
    pattern_hbm,
    b_hbm,
    rs_hbm,
    fd_hbm,
    rhs_hbm,
    schur_hbm,
    answer_hbm,
    assign_ref,
    prob_ref,
    pattern_ref,
    rs_ref,
    fd_ref,
    rhs_ref,
    rowbuf,
    colbuf,
    lefts,
    rights,
    fac,
    pat,
    acc,
    core_in,
    part,
    near_in,
    near_sum,
    far_in,
    mine,
    block,
    out_block,
    final,
    dvec,
    msg,
    inbox,
    zmsg,
    zbox,
    tally,
    halves,
    msg_half,
    inbox_half,
    tally_half,
    in_sem,
    g_send,
    g_recv,
    c_send,
    c_recv,
    na_send,
    na_recv,
    fa_send,
    fa_recv,
    fb_send,
    fb_recv,
    nb_send,
    nb_recv,
    o_send,
    o_recv,
    m_send,
    m_recv,
    z_send,
    z_recv,
    present_sem,
):
    scen = lax.axis_index("scen")
    grp = lax.axis_index("grp")
    z = scen // 2
    c = lax.rem(scen, 2)
    x = grp // SIDE
    y = lax.rem(grp, SIDE)

    def at(xx, yy, zz, cc):
        return (2 * zz + cc, SIDE * xx + yy)

    def up(v, by, n):
        return lax.rem(v + by, n)

    def remote(src, dst, send, recv, dev):
        return pltpu.make_async_remote_copy(
            src_ref=src, dst_ref=dst, send_sem=send, recv_sem=recv, device_id=dev, device_id_type=MESH
        )

    def landed(like, sem):
        pltpu.make_async_copy(like, like, sem).wait()

    fetch_tiles = tuple(pltpu.make_async_copy(b_hbm.at[k], colbuf.at[0, k], in_sem.at[k]) for k in range(KS))
    fetch_small = tuple(
        pltpu.make_async_copy(src, dst, in_sem.at[KS + i])
        for i, (src, dst) in enumerate(
            (
                (assign_hbm, assign_ref),
                (prob_hbm, prob_ref),
                (pattern_hbm, pattern_ref),
                (rs_hbm, rs_ref),
                (fd_hbm, fd_ref),
                (rhs_hbm, rhs_ref),
                (b_hbm, rowbuf.at[0]),
            )
        )
    )
    xs = [x] + [up(x, by, SIDE) for by in (1, 2, 3)]
    ys = [y] + [up(y, by, SIDE) for by in (1, 2, 3)]
    far_first = sorted(((a, b) for a in range(4) for b in range(4)), key=lambda d: -(min(d[0], 4 - d[0]) + min(d[1], 4 - d[1])))
    plane = []
    for dx, dy in far_first:
        for cc in (c, 1 - c):
            if (dx, dy) != (0, 0) or cc is not c:
                plane.append(at(xs[dx], ys[dy], z, cc))
    deep = {by: at(x, y, up(z, by, DEPTH), c) for by in range(1, DEPTH)}

    ring = [at(xs[1], y, z, c), at(xs[3], y, z, c), at(x, ys[1], z, c), at(x, ys[3], z, c)]

    with jax.named_scope("entry"):
        barrier = pltpu.get_barrier_semaphore()
        first = ring + [at(x, y, z, 1 - c), deep[1], deep[15]]
        for peer in first:
            pl.semaphore_signal(barrier, inc=1, device_id=peer, device_id_type=MESH)
        for copy in fetch_tiles + fetch_small:
            copy.start()
        pl.semaphore_wait(barrier, len(first))

    x_next, x_prev, y_next, y_prev = at(xs[1], y, z, c), at(xs[3], y, z, c), at(x, ys[1], z, c), at(x, ys[3], z, c)
    lo, hi = pl.ds(0, HALF), pl.ds(HALF, HALF)

    def hop(buf, kind, src, dst, k, rows, dev):
        return remote(buf.at[src, k, rows], buf.at[dst, k, rows], g_send.at[kind], g_recv.at[kind, k], dev)

    every = pl.ds(0, R)

    def own(k):
        return (
            hop(colbuf, 0, 0, 2, k, every, x_next),
            hop(colbuf, 0, 0, 1, k, every, x_prev),
            remote(colbuf.at[0, k], rowbuf.at[2, k], g_send.at[0], g_recv.at[0, k], y_next),
            remote(colbuf.at[0, k], rowbuf.at[1, k], g_send.at[0], g_recv.at[0, k], y_prev),
        )

    def onward(k):
        return (
            hop(colbuf, 1, 2, 3, k, lo, x_next),
            hop(colbuf, 1, 1, 3, k, hi, x_prev),
            hop(rowbuf, 1, 2, 3, k, lo, y_next),
            hop(rowbuf, 1, 1, 3, k, hi, y_prev),
        )

    for k in range(KS):
        fetch_tiles[k].wait()
        for copy in own(k):
            copy.start()

    def vouch(turn):
        peers = list(ring)
        if turn < 3:
            peers += [deep[2**turn], deep[DEPTH - 2**turn]]
        for i, peer in enumerate(peers):
            sem = present_sem.at[turn] if i < 4 else present_sem.at[4 + turn]
            pl.semaphore_signal(sem, inc=1, device_id=peer, device_id_type=MESH)

    def vouched(turn):
        pl.semaphore_wait(present_sem.at[turn], 4)
        if turn < 3:
            pl.semaphore_wait(present_sem.at[4 + turn], 2)

    vouch(0)

    with jax.named_scope("setup"):
        for copy in fetch_small:
            copy.wait()
        across = jnp.transpose(jnp.concatenate([rs_ref[...], jnp.zeros((2, R), F32)], axis=0))
        slots = lax.broadcasted_iota(jnp.int32, (1, SCEN), 1)
        present = pattern_ref[...].astype(F32)
        for k in range(KS):
            held = (slots == assign_ref[:, k : k + 1]).astype(F32)
            weight = jnp.sum(prob_ref[...] * held, axis=1, keepdims=True) / SCEN
            fac[k] = jnp.broadcast_to(across[:, k : k + 1] * weight, (R, T))
            pat[k] = jnp.broadcast_to(jnp.sum(present * held, axis=1, keepdims=True), (16, T))
        acc[...] = jnp.zeros_like(acc)

    def masked(p, k):
        keep = pat[k, pl.ds(SIDE * x + ys[REL[p]], 1), :].astype(BF16)
        return rowbuf[p, k] * keep

    def scaled(p, k):
        keep = pat[k, pl.ds(SIDE * xs[REL[p]] + y, 1), :]
        return (colbuf[p, k].astype(F32) * keep * fac[k]).astype(BF16)

    def product(left, right):
        return lax.dot_general(left, right, (((0,), (0,)), ((), ())), preferred_element_type=F32)

    def gain(value, rows, cols):
        for i, pr in enumerate(rows):
            for j, pc in enumerate(cols):
                for h in range(2):
                    for s in range(8):
                        r0 = T * i + 64 * h + SUB * s
                        acc[INDEX[pr, pc], h, s] += value[r0 : r0 + SUB, T * j : T * j + T]

    def step_a(k, carry):
        landed(colbuf.at[:, k], g_recv.at[0, k])
        for copy in onward(k):
            copy.start()
        for p in range(NEAR):
            lefts[k, :, T * p : T * p + T] = masked(p, k)
            rights[k, :, T * p : T * p + T] = scaled(p, k)
        gain(product(lefts[k], rights[k]), range(NEAR), range(NEAR))
        for turn in range(4):

            @pl.when(k == turn + 1)
            def _():
                vouched(turn)
                if turn < 3:
                    vouch(turn + 1)

        return carry

    def step_b(k, carry):
        landed(colbuf.at[pl.ds(0, 2), k], g_recv.at[1, k])
        left, right = masked(3, k), scaled(3, k)
        gain(product(left, jnp.concatenate([rights[k], right], axis=1)), (3,), range(4))
        gain(product(lefts[k], right), range(NEAR), (3,))
        return carry

    m = lax.rem(z, 4)
    q = z // 4
    ms = [m] + [up(m, by, 4) for by in (1, 2, 3)]
    qs = [q] + [up(q, by, 4) for by in (1, 2, 3)]
    front, back = pl.ds(0, 2), pl.ds(2, 2)

    def swap(w):
        tiles = pl.ds(EACH * w, EACH)
        return remote(acc.at[tiles, 1 - c], core_in.at[tiles], c_send, c_recv.at[w], at(x, y, z, 1 - c))

    def combine(w):
        swap(w).wait_recv()
        for i in range(4):
            tile, s = EACH * w + i // 2, pl.ds(4 * (i % 2), 4)
            part[w, i] = acc[tile, c, s] + core_in[tile, s]

    def near(w):
        return (
            remote(part.at[w, :, ms[1]], near_in.at[w, 0], na_send, na_recv.at[w], deep[1]),
            remote(part.at[w, :, ms[3]], near_in.at[w, 1], na_send, na_recv.at[w], deep[15]),
            remote(part.at[w, front, ms[2]], near_in.at[w, 2, front], na_send, na_recv.at[w], deep[2]),
            remote(part.at[w, back, ms[2]], near_in.at[w, 2, back], na_send, na_recv.at[w], deep[14]),
        )

    def near_done(w):
        landed(near_in.at[w], na_recv.at[w])
        near_sum[w] = part[w, :, m] + near_in[w, 0] + near_in[w, 1] + near_in[w, 2]

    def far(w):
        return tuple(
            remote(near_sum.at[w, qs[s]], far_in.at[w, s - 1], fa_send, fa_recv.at[w], deep[4 * s]) for s in (1, 2, 3)
        )

    def far_done(w):
        landed(far_in.at[w], fa_recv.at[w])
        total = near_sum[w, q] + far_in[w, 0] + far_in[w, 1] + far_in[w, 2]
        if w == 0:
            lane = lax.broadcasted_iota(jnp.int32, (SUB, T), 1)
            row = lax.broadcasted_iota(jnp.int32, (SUB, T), 0)
            diag = jnp.broadcast_to(fd_ref[x, pl.ds(y, 1), :], (SUB, T))
            spot = jnp.where(z < 8, row + 64 * c + SUB * z, -1)
            total = total + jnp.where(lane == spot, diag, 0.0)
        mine[w] = total
        block[w, q, m] = total

    def spread(w):
        return tuple(remote(mine.at[w], block.at[w, q, m], fb_send, fb_recv.at[w], deep[4 * s]) for s in (1, 2, 3))

    def share(w):
        return tuple(
            remote(block.at[w, sel, m], block.at[w, sel, m], nb_send, nb_recv.at[w], deep[by])
            for sel, by in ((pl.ds(0, 4), 1), (pl.ds(0, 4), 15), (front, 2), (back, 14))
        )

    def start(copies):
        for copy in copies:
            copy.start()

    def total_of(v):
        for axis in range(v.ndim):
            v = jnp.sum(v, axis=axis, keepdims=True)
        return v

    def share_of(tile, pieces, d_row):
        lines = []
        for pr in range(4):
            stack = []
            for piece in pieces:
                prod = None
                for pc in range(4):
                    term = tile(INDEX[pr, pc], piece) * d_row(xs[REL[pc]])
                    prod = term if prod is None else prod + term
                stack.append(prod)
            both = jnp.concatenate(stack, axis=0)
            if len(pieces) == 8:
                odd = lax.rem(ys[REL[pr]], 2)
                both = jnp.concatenate([jnp.where(odd == h, both, jnp.zeros_like(both)) for h in range(2)], axis=0)
            lines.append(jnp.sum(jnp.transpose(both), axis=0, keepdims=True))
        return lines

    def write_lines(ref, it, lines):
        for pr in range(4):
            ref[it, pl.ds(ys[REL[pr]], 1), :] = lines[pr]

    def tell(it):
        for peer in plane:
            remote(msg.at[it], inbox.at[it, 2 * y + c, x], m_send.at[it], m_recv.at[it], peer).start()
        inbox[it, 2 * y + c, x] = msg[it]

    def heard(it):
        landed(tally, m_recv.at[it])
        image = inbox[it, 0]
        for i in range(1, 8):
            image = image + inbox[it, i]
        return image

    deep_tally = tally.at[pl.ds(0, DEPTH - 1)]

    def early_begin(it, state):
        dvec[...] = state[2]
        lines = share_of(lambda i, p: acc[i, p // 8, p % 8], range(16), lambda xx: dvec[xx, pl.ds(y, 1), :])
        write_lines(zmsg, it, lines)
        for by in (8, 7, 9, 6, 10, 5, 11, 4, 12, 3, 13, 2, 14, 1, 15):
            remote(zmsg.at[it], zbox.at[it, z], z_send.at[it], z_recv.at[it], deep[by]).start()
        zbox[it, z] = zmsg[it]

    def early_middle(it):
        landed(deep_tally, z_recv.at[it])
        total = zbox[it, 0]
        for i in range(1, DEPTH):
            total = total + zbox[it, i]
        msg[it] = total
        tell(it)

    def update(it, state, image):
        answer, residual, direction, norm_now = state
        alpha = norm_now / total_of(direction * image)
        answer = answer + alpha * direction
        if it == ITERS - 1:
            return answer, residual, direction, norm_now
        residual = residual - alpha * image
        norm_next = total_of(residual * residual)
        return answer, residual, residual + (norm_next / norm_now) * direction, norm_next

    def early_end(it, state):
        return update(it, state, heard(it) + fd_ref[...] * state[2])

    early, late = range(PARTS // 2), range(PARTS // 2, PARTS)
    with jax.named_scope("gather_a"):
        lax.fori_loop(0, KS, step_a, 0)
    for w in early:
        swap(w).start()
    with jax.named_scope("gather_b0"):
        lax.fori_loop(0, 1, step_b, 0)
    with jax.named_scope("swap_a"):
        for w in early:
            combine(w)
            start(near(w))
    with jax.named_scope("gather_b1"):
        lax.fori_loop(1, 4, step_b, 0)
    with jax.named_scope("near_a0"):
        for w in early[:2]:
            near_done(w)
            start(far(w))
    with jax.named_scope("gather_b2"):
        lax.fori_loop(4, 5, step_b, 0)
    with jax.named_scope("near_a1"):
        for w in early[2:]:
            near_done(w)
            start(far(w))
    with jax.named_scope("gather_b3"):
        lax.fori_loop(5, KS, step_b, 0)
    for w in late:
        swap(w).start()
    with jax.named_scope("begin_0"):
        rhs = rhs_ref[...]
        state = (jnp.zeros_like(rhs), rhs, rhs, total_of(rhs * rhs))
        early_begin(0, state)
    with jax.named_scope("swap_b"):
        for w in late:
            combine(w)
            start(near(w))
    with jax.named_scope("middle_0"):
        early_middle(0)
    with jax.named_scope("near_b"):
        for w in late:
            near_done(w)
            start(far(w))
    with jax.named_scope("far_a"):
        for w in early:
            far_done(w)
            start(spread(w))
    with jax.named_scope("end_0"):
        state = early_end(0, state)
        early_begin(1, state)
    with jax.named_scope("far_b"):
        for w in late:
            far_done(w)
            start(spread(w))
    with jax.named_scope("spread_a"):
        for w in early:
            landed(far_in.at[w], fb_recv.at[w])
            start(share(w))
    with jax.named_scope("middle_1"):
        early_middle(1)
    with jax.named_scope("spread_b"):
        for w in late:
            landed(far_in.at[w], fb_recv.at[w])
            start(share(w))
    with jax.named_scope("end_1"):
        state = early_end(1, state)
    with jax.named_scope("share_all"):
        for w in range(PARTS):
            landed(near_in.at[w], nb_recv.at[w])

    rel = lax.rem(m + SIDE - y, SIDE)
    out_row = jnp.where(rel == 2, 3, jnp.where(rel == 3, 2, rel))
    giver = x == q
    store_schur = (pltpu.make_async_copy(out_block, schur_hbm, in_sem.at[0]),)
    store_answer = pltpu.make_async_copy(final, answer_hbm, in_sem.at[2])

    def out_tile(pc):
        idx = INDEX[0, pc]
        for pr in (1, 2, 3):
            idx = jnp.where(out_row == pr, INDEX[pr, pc], idx)
        return idx // EACH, pl.ds(2 * lax.rem(idx, EACH), 2)

    def give(pc):
        w, t = out_tile(pc)
        dev = at(xs[REL[pc]], y, z, c)
        return remote(block.at[w, t], out_block, o_send, o_recv, dev)

    def split(v):
        for p in range(2):
            for i in range(2):
                halves[p, :, i : i + 1, :] = v[:, 2 * i + p : 2 * i + p + 1, :]
        return halves[...]

    low = lax.broadcasted_iota(jnp.int32, (SIDE, 2, T), 2) < 64

    def heard_halves(n, it):
        landed(tally_half, m_recv.at[it])
        ours = []
        for cc in range(2):
            total = inbox_half[n, cc]
            for i in range(1, SIDE):
                total = total + inbox_half[n, 2 * i + cc]
            ours.append(total)
        turned = [pltpu.roll(v, 64, axis=2) for v in ours]
        return jnp.stack([jnp.where(low, ours[0], turned[1]), jnp.where(low, turned[0], ours[1])])

    state = tuple(split(v) for v in state[:3]) + (state[3].reshape(1, 1, 1, 1),)
    for n, it in enumerate(range(EARLY, ITERS)):
        with jax.named_scope(f"cg{it}"):
            halves[...] = state[2]
            lines = share_of(
                lambda i, p: block[i // 2, 2 * (i % 2) + p // 4, p % 4],
                range(8),
                lambda xx: halves[lax.rem(y, 2), xx, pl.ds(y // 2, 1), :],
            )
            write_lines(msg, it, lines)
            for i in range(2):
                msg_half[n, i : i + 1] = msg[it, 2 * i : 2 * i + 1] + msg[it, 2 * i + 1 : 2 * i + 2]
            for peer in plane:
                remote(msg_half.at[n], inbox_half.at[n, 2 * y + c, x], m_send.at[it], m_recv.at[it], peer).start()
            inbox_half[n, 2 * y + c, x] = msg_half[n]
            if it == ITERS - 1:

                @pl.when(giver)
                def _():
                    for pc in (1, 2, 3):
                        give(pc).start()
                    w, t = out_tile(0)
                    out_block[...] = block[w, t]

                @pl.when(jnp.logical_not(giver))
                def _():
                    give(1).wait_recv()

                start(store_schur)
            state = update(it, state, heard_halves(n, it))
    for xx in range(SIDE):
        for i in range(2):
            for p in range(2):
                row = 4 * (xx % 2) + 2 * i + p
                final[xx // 2, row : row + 1, :] = state[0][p, xx, i : i + 1, :]
    store_answer.start()

    with jax.named_scope("finish"):
        landed(colbuf, g_send.at[0])
        landed(colbuf.at[pl.ds(0, 2)], g_send.at[1])
        landed(core_in, c_send)
        landed(near_in, na_send)
        landed(far_in, fa_send)
        landed(far_in, fb_send)
        landed(near_in, nb_send)
        for it in range(ITERS):
            landed(tally if it < EARLY else tally_half, m_send.at[it])
        for it in range(EARLY):
            landed(deep_tally, z_send.at[it])

        @pl.when(giver)
        def _():
            landed(near_in.at[pl.ds(0, 2)], o_send)

        for copy in store_schur + (store_answer,):
            copy.wait()


def on_device(borders, row_scale, assign, prob, pattern, first_diag, rhs):
    held = pl.BlockSpec(memory_space=pltpu.HBM)
    dma = pltpu.SemaphoreType.DMA
    schur, answer = pl.pallas_call(
        kernel,
        out_shape=(
            jax.ShapeDtypeStruct((2, 4, SUB, T), F32),
            jax.ShapeDtypeStruct((2, 8, T), F32),
        ),
        in_specs=[held] * 7,
        out_specs=(held, held),
        scratch_shapes=[
            pltpu.VMEM((1, KS), jnp.int32),
            pltpu.VMEM((1, SCEN), F32),
            pltpu.VMEM((16, SCEN), jnp.int32),
            pltpu.VMEM((KS, R), F32),
            pltpu.VMEM((SIDE, SIDE, T), F32),
            pltpu.VMEM((SIDE, SIDE, T), F32),
            pltpu.VMEM((4, KS, R, T), BF16),
            pltpu.VMEM((4, KS, R, T), BF16),
            pltpu.VMEM((KS, R, NEAR * T), BF16),
            pltpu.VMEM((KS, R, NEAR * T), BF16),
            pltpu.VMEM((KS, R, T), F32),
            pltpu.VMEM((KS, 16, T), F32),
            pltpu.VMEM((16, 2, 8, SUB, T), F32),
            pltpu.VMEM((16, 8, SUB, T), F32),
            pltpu.VMEM((PARTS, 4, 4, SUB, T), F32),
            pltpu.VMEM((PARTS, 3, 4, SUB, T), F32),
            pltpu.VMEM((PARTS, 4, SUB, T), F32),
            pltpu.VMEM((PARTS, 3, SUB, T), F32),
            pltpu.VMEM((PARTS, SUB, T), F32),
            pltpu.VMEM((PARTS, 4, 4, SUB, T), F32),
            pltpu.VMEM((2, 4, SUB, T), F32),
            pltpu.VMEM((2, 8, T), F32),
            pltpu.VMEM((SIDE, SIDE, T), F32),
            pltpu.VMEM((ITERS, SIDE, T), F32),
            pltpu.VMEM((EARLY, 8, SIDE, SIDE, T), F32),
            pltpu.VMEM((EARLY, SIDE, T), F32),
            pltpu.VMEM((EARLY, DEPTH, SIDE, T), F32),
            pltpu.VMEM((31, SIDE, T), F32),
            pltpu.VMEM((2, SIDE, 2, T), F32),
            pltpu.VMEM((ITERS - EARLY, 2, T), F32),
            pltpu.VMEM((ITERS - EARLY, 8, SIDE, 2, T), F32),
            pltpu.VMEM((31, 2, T), F32),
            dma((KS + 7,)),
            dma((2,)),
            dma((2, KS)),
            dma,
            dma((PARTS,)),
            dma,
            dma((PARTS,)),
            dma,
            dma((PARTS,)),
            dma,
            dma((PARTS,)),
            dma,
            dma((PARTS,)),
            dma,
            dma,
            dma((ITERS,)),
            dma((ITERS,)),
            dma((EARLY,)),
            dma((EARLY,)),
            pltpu.SemaphoreType.REGULAR((7,)),
        ],
        compiler_params=pltpu.CompilerParams(
            collective_id=0, has_side_effects=True, vmem_limit_bytes=67_043_328
        ),
    )(
        assign.reshape(1, KS),
        prob.reshape(1, SCEN),
        pattern.T,
        borders,
        row_scale,
        first_diag.reshape(SIDE, SIDE, T),
        rhs.reshape(SIDE, SIDE, T),
    )
    return schur.reshape(8 * SUB, T), answer.reshape(SIDE * SIDE * T)


def solution(mesh):
    placed = (P("scen", None, "grp"), P("scen", None), P("scen"), P(), P(), P(), P())
    return jax.shard_map(
        on_device, mesh=mesh, in_specs=placed, out_specs=(P("scen", "grp"), P()), check_vma=False
    )
```
